32 devices in a mesh: dp: 8 (over y, x, core), tensor: 4 (over z).
Axes of the slice: x: 2, y: 2, z: 4, core: 2. Of those that a mesh axis runs over, the one named last changes fastest.
Arguments:
- tokens: bfloat16 [8, 1024, 2048], P('dp'), may hold values from -6 to 6
- cotangent: bfloat16 [8, 1024, 2048], P('dp'), may hold values from -6 to 6
- lengths: int32 [8], P('dp'), may hold values from 128 to 1024, as said below
- keep: int32 [8, 1024], P('dp'), may hold values 0 or 1
- first_gain: float32 [2048], replicated, may hold values from 0.25 to 1.75
- first_shift: float32 [2048], replicated, may hold values from -3 to 3
- second_gain: float32 [2048], replicated, may hold values from 0.25 to 1.75
- second_shift: float32 [2048], replicated, may hold values from -3 to 3
- qkv_weight: bfloat16 [8, 768, 2048], P('tensor', 'dp'), may hold values from -0.125 to 0.125
- qkv_bias: bfloat16 [8, 768], P('tensor', 'dp'), may hold values from -3 to 3
- dense_weight: bfloat16 [8, 256, 2048], P('tensor', 'dp'), may hold values from -1 to 1
- up_weight: bfloat16 [8192, 2048], P(('dp', 'tensor')), may hold values from -0.125 to 0.125
- up_bias: bfloat16 [8192], P(('dp', 'tensor')), may hold values from -3 to 3
- down_weight: bfloat16 [8192, 2048], P(('dp', 'tensor')), may hold values from -0.0625 to 0.0625
- branch_bias: float32 [2048], replicated, may hold values from -3 to 3
Outputs:
- block_out: bfloat16 [8, 1024, 2048], P('dp', None, 'tensor')
- input_grad: bfloat16 [8, 1024, 2048], P('dp', None, 'tensor')
- qkv_weight_grad: float32 [8, 768, 2048], P('tensor', 'dp')
- qkv_bias_grad: float32 [8, 768], P('tensor', 'dp')
- dense_weight_grad: float32 [8, 256, 2048], P('tensor', 'dp')
- up_weight_grad: float32 [8192, 2048], P(('dp', 'tensor'))
- up_bias_grad: float32 [8192], P(('dp', 'tensor'))
- down_weight_grad: float32 [8192, 2048], P(('dp', 'tensor'))
- norm_grads: float32 [5, 2048], P(None, ('dp', 'tensor'))
The draws below stay inside these ranges and needn't reach their ends.
Inputs may be any that keep to these rules, and one draw needn't show every extreme that they name: Each sequence's valid tokens are its first lengths; one sequence has exactly 1024 and one exactly 128.
All inputs are finite; a program needn't handle non-finite values. No bound on the sum of `keep` on one device may be relied on, other than what follows from the above.
Results may differ from the reference program's by a relative error of at most 0.015.
Values may be sent and summed in bfloat16 or wider, within the bound.
A program may use at most 320 MiB of HBM per device.

```python
import jax
import jax.numpy as jnp
from jax import lax

D = 2048
HEADS = 8
HEAD = 256
ROT = 64
FF = 8192
LEN = 1024
MIN_LEN = 128
BLOCK = 512
SEQS = 8


def draw_lengths(key, part):
    key_lengths, key_longest, key_offset = jax.random.split(key, 3)
    drawn = jax.random.randint(key_lengths, (SEQS,), MIN_LEN, LEN + 1)
    longest = jax.random.randint(key_longest, (), 0, SEQS)
    shortest = (longest + jax.random.randint(key_offset, (), 1, SEQS)) % SEQS
    drawn = drawn.at[longest].set(LEN).at[shortest].set(MIN_LEN)
    return drawn.astype(jnp.int32)


def place_ends(values, stream_key, low, largest):
    shape = values.shape
    place = [jax.random.randint(jax.random.fold_in(stream_key, axis), (), 0, shape[axis]) for axis in range(len(shape))]
    values = values.at[tuple(place)].set(low)
    longest = shape.index(max(shape))
    place[longest] = (place[longest] + 1) % shape[longest]
    return values.at[tuple(place)].set(largest)


def block_scale(rng, extent, cuts, low, largest):
    def one(axis_at, shards_of):
        heights = jax.random.uniform(jax.random.fold_in(jax.random.fold_in(rng, 6), axis_at), (shards_of,), jnp.float32, low / len(cuts), largest / len(cuts))
        return jnp.repeat(jnp.exp(heights), extent[axis_at] // shards_of).reshape((-1,) + (1,) * (len(extent) - axis_at - 1))

    level = one(*cuts[0])
    for cut in cuts[1:]:
        level = level * one(*cut)
    return level


def bell_draw(rng, shape, deviation, bound, shards=(), kind=jnp.bfloat16):
    level = block_scale(rng, shape, shards, -0.22, 0.18) if shards else 1.0
    entries = jax.random.normal(rng, shape, jnp.float32) * deviation * level
    return jnp.minimum(jnp.maximum(entries, -bound), bound).astype(kind)


def setup_inputs(seed: int = 0) -> dict:
    splits = jax.random.split(jax.random.key(seed), 16)
    tokens = bell_draw(splits[0], (SEQS, LEN, D), 1.0, 6.0, ((0, 8),))
    cotangent = bell_draw(splits[1], (SEQS, LEN, D), 1.0, 6.0, ((0, 8),))
    lengths = draw_lengths(jax.random.fold_in(splits[15], 71), 0)
    keep = place_ends((jax.random.randint(splits[3], (SEQS, LEN), 0, 8) < 7).astype(jnp.int32), jax.random.fold_in(splits[3], 1), 0, 1)
    first_gain = jnp.clip(1.0 + 0.15 * jax.random.normal(splits[4], (D,), jnp.float32), 0.25, 1.75)
    first_shift = bell_draw(splits[5], (D,), 0.3, 3.0, (), jnp.float32)
    second_gain = jnp.clip(1.0 + 0.15 * jax.random.normal(splits[6], (D,), jnp.float32), 0.25, 1.75)
    second_shift = bell_draw(splits[7], (D,), 0.3, 3.0, (), jnp.float32)
    qkv_weight = bell_draw(splits[8], (HEADS, 3 * HEAD, D), D ** -0.5, 0.125, ((0, 4), (1, 8)))
    qkv_bias = bell_draw(splits[9], (HEADS, 3 * HEAD), 0.3, 3.0, ((0, 4), (1, 8)))
    dense_weight = bell_draw(splits[10], (HEADS, HEAD, D), (D // 64) ** -0.5, 1.0, ((0, 4), (1, 8)))
    up_weight = bell_draw(splits[11], (FF, D), D ** -0.5, 0.125, ((0, 32),))
    up_bias = bell_draw(splits[12], (FF,), 0.5, 3.0, ((0, 32),))
    down_weight = bell_draw(splits[13], (FF, D), FF ** -0.5, 0.0625, ((0, 32),))
    branch_bias = bell_draw(splits[14], (D,), 0.5, 3.0, (), jnp.float32)
    return {"tokens": tokens, "cotangent": cotangent, "lengths": lengths, "keep": keep, "first_gain": first_gain, "first_shift": first_shift, "second_gain": second_gain, "second_shift": second_shift, "qkv_weight": qkv_weight, "qkv_bias": qkv_bias, "dense_weight": dense_weight, "up_weight": up_weight, "up_bias": up_bias, "down_weight": down_weight, "branch_bias": branch_bias}


@jax.custom_vjp
def low(v):
    return lax.optimization_barrier(v.astype(jnp.bfloat16)).astype(jnp.float32)

@jax.custom_vjp
def low_back(v):
    return v

def low_keep(v):
    return (low(v), None)

def low_pass(kept, grad):
    return (grad,)

def back_keep(v):
    return (v, None)

def back_low(kept, grad):
    return (low(grad),)
low.defvjp(low_keep, low_pass)
low_back.defvjp(back_keep, back_low)

def layer_norm(values, gain, shift):
    centred = values - lax.optimization_barrier(jnp.mean(values, axis=-1, keepdims=True))
    spread = lax.optimization_barrier(jnp.mean(centred * centred, axis=-1, keepdims=True))
    return centred * lax.rsqrt(spread + 1e-05) * gain + shift

def rotary_tables(start, count):
    half = ROT // 2
    inverse = 10000.0 ** (-jnp.arange(half, dtype=jnp.float32) * 2.0 / ROT)
    angles = (start + jnp.arange(count, dtype=jnp.float32))[:, None] * inverse[None, :]
    angles = jnp.concatenate([angles, angles], axis=1)
    return (jnp.cos(angles)[:, None, :], jnp.sin(angles)[:, None, :])

def rotate(values, cosine, sine):
    half = ROT // 2
    part = values[..., :ROT]
    turned = jnp.concatenate([-part[..., half:], part[..., :half]], axis=-1)
    return jnp.concatenate([part * cosine + turned * sine, values[..., ROT:]], axis=-1)

def attend_block(query_block, start, keys, values, length):
    highest = lax.Precision.HIGHEST
    scores = jnp.einsum('qhe,khe->hqk', query_block, keys, precision=highest) * HEAD ** (-0.5)
    scores = low_back(scores)
    rows = start + jnp.arange(BLOCK).astype(jnp.int32)
    columns = jnp.arange(LEN).astype(jnp.int32)
    allowed = (columns[None, :] <= rows[:, None]) & (columns[None, :] < length)
    scores = jnp.where(allowed[None], scores, -1e+30)
    peak = lax.optimization_barrier(jnp.max(scores, axis=-1, keepdims=True))
    weights = jnp.exp(scores - peak)
    probs = low(weights / lax.optimization_barrier(jnp.sum(weights, axis=-1, keepdims=True)))
    result = jnp.einsum('hqk,khe->qhe', probs, values, precision=highest)
    return low(low_back(result))

def forward(tokens, length, first_gain, first_shift, second_gain, second_shift, qkv_weight, qkv_bias, dense_weight, up_weight, up_bias, down_weight, branch_bias):
    highest = lax.Precision.HIGHEST
    normed = low(layer_norm(tokens, first_gain, first_shift))
    joint = jnp.einsum('ld,hed->lhe', normed, qkv_weight, precision=highest) + qkv_bias[None]
    joint = low_back(joint)
    cosine, sine = rotary_tables(0, LEN)
    query = low(rotate(joint[..., :HEAD], cosine, sine))
    keys = low(rotate(joint[..., HEAD:2 * HEAD], cosine, sine))
    values = low(joint[..., 2 * HEAD:])
    checked = jax.checkpoint(attend_block)
    query_blocks = query.reshape(LEN // BLOCK, BLOCK, HEADS, HEAD)
    starts = (jnp.arange(LEN // BLOCK) * BLOCK).astype(jnp.int32)
    attended = lax.map(lambda item: checked(item[0], item[1], keys, values, length), (query_blocks, starts))
    attended = attended.reshape(LEN, HEADS, HEAD)
    attention = jnp.einsum('lhe,hed->ld', attended, dense_weight, precision=highest)
    mixed = low(layer_norm(tokens, second_gain, second_shift))
    hidden = low_back(jnp.einsum('ld,fd->lf', mixed, up_weight, precision=highest) + up_bias)
    active = low(jax.nn.gelu(hidden, approximate=False))
    feed = jnp.dot(active, down_weight, precision=highest)
    live = (jnp.arange(LEN).astype(jnp.int32) < length).astype(jnp.float32)[:, None]
    return tokens + live * (attention + feed + branch_bias)

def reference(tokens, cotangent, lengths, keep, first_gain, first_shift, second_gain, second_shift, qkv_weight, qkv_bias, dense_weight, up_weight, up_bias, down_weight, branch_bias):
    weights = tuple((item.astype(jnp.float32) for item in (first_gain, first_shift, second_gain, second_shift, qkv_weight, qkv_bias, dense_weight, up_weight, up_bias, down_weight, branch_bias)))

    def one_sequence(totals, items):
        row_tokens, row_grad, length, row_keep = items
        positions = jnp.arange(LEN).astype(jnp.int32)
        valid = ((positions < length) & (row_keep == 1)).astype(jnp.float32)
        grad_rows = row_grad.astype(jnp.float32) * valid[:, None]

        def run(values, *weights_now):
            return forward(values, length, *weights_now)
        result, pullback = jax.vjp(run, row_tokens.astype(jnp.float32), *weights)
        grads = pullback(grad_rows)
        totals = tuple((total + grad for total, grad in zip(totals, grads[1:])))
        return (totals, (result.astype(jnp.bfloat16), grads[0].astype(jnp.bfloat16)))
    initial = tuple((jnp.zeros_like(item) for item in weights))
    totals, outputs = lax.scan(one_sequence, initial, (tokens, cotangent, lengths, keep))
    norm_grads = jnp.stack([totals[0], totals[1], totals[2], totals[3], totals[10]])
    return (outputs[0], outputs[1], totals[4], totals[5], totals[6], totals[7], totals[8], totals[9], norm_grads)
```

```python
from functools import partial

import jax
import jax.numpy as jnp
from jax import lax
from jax.experimental import pallas as pl
from jax.experimental.pallas import tpu as pltpu
from jax.sharding import PartitionSpec as P

HEAD = 256
ROT = 64
BLOCK = 512


def layer_norm_parts(values, gain, shift):
    centred = values - jnp.mean(values, axis=-1, keepdims=True)
    inverse = lax.rsqrt(jnp.mean(centred * centred, axis=-1, keepdims=True) + 1e-05)
    unit = centred * inverse
    return (unit * gain + shift, unit, inverse)


def norm_back(grad, unit, inverse, gain):
    scaled = grad * gain
    centred = scaled - jnp.mean(scaled, axis=-1, keepdims=True)
    return inverse * (centred - unit * jnp.mean(scaled * unit, axis=-1, keepdims=True))


def rotary_tables(start, count):
    half = ROT // 2
    inverse = 10000.0 ** (-jnp.arange(half, dtype=jnp.float32) * 2.0 / ROT)
    angles = (start + jnp.arange(count, dtype=jnp.float32))[:, None] * inverse[None, :]
    angles = jnp.concatenate([angles, angles], axis=1)
    return (jnp.cos(angles)[:, None, :], jnp.sin(angles)[:, None, :])


def rotate(values, cosine, sine):
    half = ROT // 2
    part = values[..., :ROT]
    turned = jnp.concatenate([-part[..., half:], part[..., :half]], axis=-1)
    return jnp.concatenate([part * cosine + turned * sine, values[..., ROT:]], axis=-1)


def rotate_back(grad, cosine, sine):
    half = ROT // 2
    part = grad[..., :ROT]
    scaled = part * sine
    turned = jnp.concatenate([scaled[..., half:], -scaled[..., :half]], axis=-1)
    return jnp.concatenate([part * cosine + turned, grad[..., ROT:]], axis=-1)


def block_scores(query_block, key_rows, query_start, key_start, length):
    scores = jnp.einsum(
        "qhe,khe->hqk", query_block, key_rows, preferred_element_type=jnp.float32
    ) * HEAD ** (-0.5)
    rows = query_start + jnp.arange(query_block.shape[0])
    columns = key_start + jnp.arange(key_rows.shape[0])
    allowed = (columns[None, :] <= rows[:, None]) & (columns[None, :] < length)
    return jnp.where(allowed[None], scores, -1e30)


def when_live(flag, work, operand):
    return lax.cond(flag, work, lambda unused: jax.tree.map(jnp.zeros_like, work(unused)), operand)


def local_general(
    tokens,
    cotangent,
    lengths,
    keep,
    first_gain,
    first_shift,
    second_gain,
    second_shift,
    qkv_weight,
    qkv_bias,
    dense_weight,
    up_weight,
    up_bias,
    down_weight,
    branch_bias,
):
    gathered = (
        lax.all_gather(qkv_weight, "dp", axis=1, tiled=True),
        lax.all_gather(qkv_bias, "dp", axis=1, tiled=True),
        lax.all_gather(dense_weight, "dp", axis=1, tiled=True),
        lax.all_gather(up_weight, "dp", axis=0, tiled=True),
        lax.all_gather(up_bias, "dp", axis=0, tiled=True),
        lax.all_gather(down_weight, "dp", axis=0, tiled=True),
    )
    qkv_full, qkv_bias_full, dense_full, up_full, up_bias_full, down_full = gathered
    seq_count, length_all, width = tokens.shape
    blocks = length_all // BLOCK
    heads_here = qkv_full.shape[0]
    hidden_here = up_full.shape[0]
    scale = HEAD ** (-0.5)
    positions = jnp.arange(length_all)
    live_rows = positions[None, :] < lengths[:, None]

    def forward_one(items):
        row_tokens, length = items
        dense_flat = dense_full.reshape(heads_here * HEAD, width)

        def project(row_block, start):
            values32 = row_block.astype(jnp.float32)
            normed = layer_norm_parts(values32, first_gain, first_shift)[0].astype(jnp.bfloat16)
            joint = jnp.einsum(
                "bd,hed->bhe", normed, qkv_full, preferred_element_type=jnp.float32
            ) + qkv_bias_full.astype(jnp.float32)
            cosine, sine = rotary_tables(start, BLOCK)
            query_rows = rotate(joint[..., :HEAD], cosine, sine).astype(jnp.bfloat16)
            key_rows = rotate(joint[..., HEAD : 2 * HEAD], cosine, sine).astype(jnp.bfloat16)
            value_rows = joint[..., 2 * HEAD :].astype(jnp.bfloat16)
            mixed = layer_norm_parts(values32, second_gain, second_shift)[0].astype(jnp.bfloat16)
            hidden_rows = jnp.einsum(
                "bd,fd->bf", mixed, up_full, preferred_element_type=jnp.float32
            ) + up_bias_full.astype(jnp.float32)
            active = jax.nn.gelu(hidden_rows, approximate=False).astype(jnp.bfloat16)
            feed = jnp.dot(active, down_full, preferred_element_type=jnp.float32)
            return (query_rows, key_rows, value_rows, hidden_rows, feed)

        outputs = []
        for index in range(blocks):
            start = index * BLOCK
            outputs.append(
                when_live(
                    start < length, partial(project, start=start), row_tokens[start : start + BLOCK]
                )
            )
        query_all = jnp.concatenate([item[0] for item in outputs], axis=0)
        keys_all = jnp.concatenate([item[1] for item in outputs], axis=0)
        values_all = jnp.concatenate([item[2] for item in outputs], axis=0)
        hidden_all = jnp.concatenate([item[3] for item in outputs], axis=0)
        feed_all = jnp.concatenate([item[4] for item in outputs], axis=0)

        def attend(query_block, start):
            peak = jnp.full((heads_here, BLOCK, 1), -1e30, jnp.float32)
            total = jnp.zeros((heads_here, BLOCK, 1), jnp.float32)
            for key_index in range(start // BLOCK + 1):
                key_start = key_index * BLOCK
                scores = block_scores(
                    query_block, keys_all[key_start : key_start + BLOCK], start, key_start, length
                )
                newer = jnp.maximum(peak, jnp.max(scores, axis=-1, keepdims=True))
                total = total * jnp.exp(peak - newer) + jnp.sum(
                    jnp.exp(scores - newer), axis=-1, keepdims=True
                )
                peak = newer
            logsum = peak + jnp.log(total)
            summed = jnp.zeros((BLOCK, heads_here, HEAD), jnp.float32)
            for key_index in range(start // BLOCK + 1):
                key_start = key_index * BLOCK
                scores = block_scores(
                    query_block, keys_all[key_start : key_start + BLOCK], start, key_start, length
                )
                probs = jnp.exp(scores - logsum).astype(jnp.bfloat16)
                summed = summed + jnp.einsum(
                    "hqk,khe->qhe",
                    probs,
                    values_all[key_start : key_start + BLOCK],
                    preferred_element_type=jnp.float32,
                )
            attended_block = summed.astype(jnp.bfloat16).reshape(BLOCK, heads_here * HEAD)
            attention_rows = jnp.dot(attended_block, dense_flat, preferred_element_type=jnp.float32)
            return (attended_block, logsum[..., 0], attention_rows)

        pieces = []
        for index in range(blocks):
            start = index * BLOCK
            pieces.append(
                when_live(
                    start < length, partial(attend, start=start), query_all[start : start + BLOCK]
                )
            )
        attended_all = jnp.concatenate([item[0] for item in pieces], axis=0)
        logsum_all = jnp.concatenate([item[1] for item in pieces], axis=1)
        attention_all = jnp.concatenate([item[2] for item in pieces], axis=0)
        live = (positions < length)[:, None]
        branch_part = jnp.where(live, attention_all + feed_all, 0.0)
        return (branch_part, query_all, keys_all, values_all, hidden_all, attended_all, logsum_all)

    branch_part, query_all, keys_all, values_all, hidden_all, attended_all, logsum_all = lax.map(
        forward_one, (tokens, lengths)
    )
    branch_total = lax.psum_scatter(branch_part, "tensor", scatter_dimension=2, tiled=True)
    slice_width = branch_total.shape[2]
    column_start = lax.axis_index("tensor") * slice_width
    token_slice = lax.dynamic_slice_in_dim(tokens, column_start, slice_width, 2).astype(jnp.float32)
    bias_slice = lax.dynamic_slice_in_dim(branch_bias, column_start, slice_width, 0)
    block_out = (
        token_slice + jnp.where(live_rows[..., None], branch_total + bias_slice, 0.0)
    ).astype(jnp.bfloat16)
    qkv_back, dense_back, up_back, down_back = (
        lax.all_gather(qkv_weight, "dp", axis=1, tiled=True),
        lax.all_gather(dense_weight, "dp", axis=1, tiled=True),
        lax.all_gather(up_weight, "dp", axis=0, tiled=True),
        lax.all_gather(down_weight, "dp", axis=0, tiled=True),
    )
    dense_back_flat = dense_back.reshape(heads_here * HEAD, width)
    valid = live_rows & (keep == 1)
    grad_out = jnp.where(valid[..., None], cotangent, jnp.zeros((), jnp.bfloat16))
    row_width = length_all // lax.axis_size("tensor")
    row_start = lax.axis_index("tensor") * row_width
    bias_term = jnp.sum(
        lax.dynamic_slice_in_dim(grad_out, row_start, row_width, 1).astype(jnp.float32), axis=(0, 1)
    )

    def feed_back(carry, items):
        row_tokens, row_grad, row_hidden, length = items
        outputs = []
        for index in range(blocks):
            start = index * BLOCK

            def work(operand, start=start):
                grad_up, grad_up_bias, grad_down, gain_two, shift_two = operand
                values32 = row_tokens[start : start + BLOCK].astype(jnp.float32)
                normed, unit, inverse = layer_norm_parts(values32, second_gain, second_shift)
                mixed = normed.astype(jnp.bfloat16)
                grad_rows = row_grad[start : start + BLOCK]
                hidden_rows = row_hidden[start : start + BLOCK]
                grad_active = jnp.einsum(
                    "bd,fd->bf", grad_rows, down_back, preferred_element_type=jnp.float32
                )
                active, gelu_back = jax.vjp(partial(jax.nn.gelu, approximate=False), hidden_rows)
                grad_hidden = gelu_back(grad_active)[0].astype(jnp.bfloat16)
                grad_down = grad_down + jnp.einsum(
                    "bf,bd->fd",
                    active.astype(jnp.bfloat16),
                    grad_rows,
                    preferred_element_type=jnp.float32,
                )
                grad_up = grad_up + jnp.einsum(
                    "bf,bd->fd", grad_hidden, mixed, preferred_element_type=jnp.float32
                )
                grad_up_bias = grad_up_bias + jnp.sum(grad_hidden.astype(jnp.float32), axis=0)
                grad_mixed = jnp.dot(grad_hidden, up_back, preferred_element_type=jnp.float32)
                gain_two = gain_two + jnp.sum(grad_mixed * unit, axis=0)
                shift_two = shift_two + jnp.sum(grad_mixed, axis=0)
                return (
                    (grad_up, grad_up_bias, grad_down, gain_two, shift_two),
                    norm_back(grad_mixed, unit, inverse, second_gain),
                )

            carry, piece = lax.cond(
                start < length,
                work,
                lambda operand: (operand, jnp.zeros((BLOCK, width), jnp.float32)),
                carry,
            )
            outputs.append(piece)
        return (carry, jnp.concatenate(outputs, axis=0))

    feed_init = (
        jnp.zeros((hidden_here, width), jnp.float32),
        jnp.zeros((hidden_here,), jnp.float32),
        jnp.zeros((hidden_here, width), jnp.float32),
        jnp.zeros((width,), jnp.float32),
        jnp.zeros((width,), jnp.float32),
    )
    feed_totals, grad_x_two = lax.scan(
        feed_back, feed_init, (tokens, grad_out, hidden_all, lengths)
    )
    grad_up_total, grad_up_bias_total, grad_down_total, gain_two, shift_two = feed_totals

    def attention_back(carry, items):
        (
            row_tokens,
            row_grad,
            query_rows,
            key_rows,
            value_rows,
            attended_rows,
            logsum_rows,
            length,
        ) = items
        grad_qkv, grad_qkv_bias, grad_dense, gain_one, shift_one = carry
        grad_attended = jnp.einsum(
            "ld,nd->ln", row_grad, dense_back_flat, preferred_element_type=jnp.float32
        ).astype(jnp.bfloat16)
        grad_dense = grad_dense + jnp.einsum(
            "ln,ld->nd", attended_rows, row_grad, preferred_element_type=jnp.float32
        )
        grad_attended = grad_attended.reshape(length_all, heads_here, HEAD)
        grad_keys = jnp.zeros((length_all, heads_here, HEAD), jnp.float32)
        grad_values = jnp.zeros((length_all, heads_here, HEAD), jnp.float32)
        query_grads = []
        for query_index in range(blocks):
            query_start = query_index * BLOCK

            def work(operand, query_start=query_start, query_index=query_index):
                grad_keys_now, grad_values_now = operand
                query_block = query_rows[query_start : query_start + BLOCK]
                grad_block = grad_attended[query_start : query_start + BLOCK]
                logsum_block = logsum_rows[:, query_start : query_start + BLOCK][..., None]

                def probs_and_grad(key_start):
                    scores = block_scores(
                        query_block,
                        key_rows[key_start : key_start + BLOCK],
                        query_start,
                        key_start,
                        length,
                    )
                    probs = jnp.exp(scores - logsum_block)
                    grad_probs = jnp.einsum(
                        "qhe,khe->hqk",
                        grad_block,
                        value_rows[key_start : key_start + BLOCK],
                        preferred_element_type=jnp.float32,
                    )
                    return (probs, grad_probs)

                delta = jnp.zeros((heads_here, BLOCK, 1), jnp.float32)
                for key_index in range(query_index + 1):
                    probs, grad_probs = probs_and_grad(key_index * BLOCK)
                    delta = delta + jnp.sum(probs * grad_probs, axis=-1, keepdims=True)
                grad_query_block = jnp.zeros((BLOCK, heads_here, HEAD), jnp.float32)
                for key_index in range(query_index + 1):
                    key_start = key_index * BLOCK
                    probs, grad_probs = probs_and_grad(key_start)
                    grad_scores = (probs * (grad_probs - delta)).astype(jnp.bfloat16)
                    grad_query_block = (
                        grad_query_block
                        + jnp.einsum(
                            "hqk,khe->qhe",
                            grad_scores,
                            key_rows[key_start : key_start + BLOCK],
                            preferred_element_type=jnp.float32,
                        )
                        * scale
                    )
                    grad_keys_now = grad_keys_now.at[key_start : key_start + BLOCK].add(
                        jnp.einsum(
                            "hqk,qhe->khe",
                            grad_scores,
                            query_block,
                            preferred_element_type=jnp.float32,
                        )
                        * scale
                    )
                    grad_values_now = grad_values_now.at[key_start : key_start + BLOCK].add(
                        jnp.einsum(
                            "hqk,qhe->khe",
                            probs.astype(jnp.bfloat16),
                            grad_block,
                            preferred_element_type=jnp.float32,
                        )
                    )
                return ((grad_keys_now, grad_values_now), grad_query_block)

            (grad_keys, grad_values), query_piece = lax.cond(
                query_start < length,
                work,
                lambda operand: (operand, jnp.zeros((BLOCK, heads_here, HEAD), jnp.float32)),
                (grad_keys, grad_values),
            )
            query_grads.append(query_piece)
        grad_query = jnp.concatenate(query_grads, axis=0)
        cosine, sine = rotary_tables(0, length_all)
        grad_joint = jnp.concatenate(
            [
                rotate_back(grad_query, cosine, sine),
                rotate_back(grad_keys, cosine, sine),
                grad_values,
            ],
            axis=-1,
        ).astype(jnp.bfloat16)
        inner = (grad_qkv, grad_qkv_bias, gain_one, shift_one)
        outputs = []
        for index in range(blocks):
            start = index * BLOCK

            def work_norm(operand, start=start):
                grad_qkv_now, grad_bias_now, gain_now, shift_now = operand
                values32 = row_tokens[start : start + BLOCK].astype(jnp.float32)
                normed, unit, inverse = layer_norm_parts(values32, first_gain, first_shift)
                grad_rows = grad_joint[start : start + BLOCK]
                grad_qkv_now = grad_qkv_now + jnp.einsum(
                    "bhe,bd->hed",
                    grad_rows,
                    normed.astype(jnp.bfloat16),
                    preferred_element_type=jnp.float32,
                )
                grad_bias_now = grad_bias_now + jnp.sum(grad_rows.astype(jnp.float32), axis=0)
                grad_normed = jnp.einsum(
                    "bhe,hed->bd", grad_rows, qkv_back, preferred_element_type=jnp.float32
                )
                gain_now = gain_now + jnp.sum(grad_normed * unit, axis=0)
                shift_now = shift_now + jnp.sum(grad_normed, axis=0)
                return (
                    (grad_qkv_now, grad_bias_now, gain_now, shift_now),
                    norm_back(grad_normed, unit, inverse, first_gain),
                )

            inner, piece = lax.cond(
                start < length,
                work_norm,
                lambda operand: (operand, jnp.zeros((BLOCK, width), jnp.float32)),
                inner,
            )
            outputs.append(piece)
        grad_qkv, grad_qkv_bias, gain_one, shift_one = inner
        return (
            (grad_qkv, grad_qkv_bias, grad_dense, gain_one, shift_one),
            jnp.concatenate(outputs, axis=0),
        )

    attention_init = (
        jnp.zeros(qkv_back.shape, jnp.float32),
        jnp.zeros((heads_here, 3 * HEAD), jnp.float32),
        jnp.zeros((heads_here * HEAD, width), jnp.float32),
        jnp.zeros((width,), jnp.float32),
        jnp.zeros((width,), jnp.float32),
    )
    attention_totals, grad_x_one = lax.scan(
        attention_back,
        attention_init,
        (tokens, grad_out, query_all, keys_all, values_all, attended_all, logsum_all, lengths),
    )
    grad_qkv_total, grad_qkv_bias_total, grad_dense_total, gain_one, shift_one = attention_totals
    grad_dense_total = grad_dense_total.reshape(heads_here, HEAD, width)
    norms_total = jnp.stack([gain_one, shift_one, gain_two, shift_two, bias_term])
    (
        qkv_grad_out,
        qkv_bias_grad_out,
        dense_grad_out,
        up_grad_out,
        up_bias_grad_out,
        down_grad_out,
        norms_dp,
    ) = (
        lax.psum_scatter(
            grad_qkv_total.astype(jnp.bfloat16), "dp", scatter_dimension=1, tiled=True
        ).astype(jnp.float32),
        lax.psum_scatter(
            grad_qkv_bias_total.astype(jnp.bfloat16), "dp", scatter_dimension=1, tiled=True
        ).astype(jnp.float32),
        lax.psum_scatter(
            grad_dense_total.astype(jnp.bfloat16), "dp", scatter_dimension=1, tiled=True
        ).astype(jnp.float32),
        lax.psum_scatter(
            grad_up_total.astype(jnp.bfloat16), "dp", scatter_dimension=0, tiled=True
        ).astype(jnp.float32),
        lax.psum_scatter(
            grad_up_bias_total.astype(jnp.bfloat16), "dp", scatter_dimension=0, tiled=True
        ).astype(jnp.float32),
        lax.psum_scatter(
            grad_down_total.astype(jnp.bfloat16), "dp", scatter_dimension=0, tiled=True
        ).astype(jnp.float32),
        lax.psum_scatter(
            norms_total.astype(jnp.bfloat16), "dp", scatter_dimension=1, tiled=True
        ).astype(jnp.float32),
    )
    grad_x_partial = grad_x_one + grad_x_two
    grad_x_total, norms_out = (
        lax.psum_scatter(grad_x_partial, "tensor", scatter_dimension=2, tiled=True),
        lax.psum_scatter(norms_dp, "tensor", scatter_dimension=1, tiled=True),
    )
    grad_slice = lax.dynamic_slice_in_dim(grad_out, column_start, slice_width, 2).astype(
        jnp.float32
    )
    input_grad = (grad_slice + grad_x_total).astype(jnp.bfloat16)
    return (
        block_out,
        input_grad,
        qkv_grad_out,
        qkv_bias_grad_out,
        dense_grad_out,
        up_grad_out,
        up_bias_grad_out,
        down_grad_out,
        norms_out,
    )


F32 = jnp.float32
LOW = jnp.bfloat16
ROWS = 512
VMEM_LIMIT = 60 * 1024 * 1024


def dot_nt(left, right):
    return lax.dot_general(left, right, (((1,), (1,)), ((), ())), preferred_element_type=F32)


def dot_nn(left, right):
    return lax.dot_general(left, right, (((1,), (0,)), ((), ())), preferred_element_type=F32)


def dot_tn(left, right):
    return lax.dot_general(left, right, (((0,), (0,)), ((), ())), preferred_element_type=F32)


def whole(shape):
    return pl.BlockSpec(shape, lambda *_: (0,) * len(shape), pipeline_mode=pl.Buffered(1))


def params(dims=1):
    return pltpu.CompilerParams(
        dimension_semantics=("arbitrary",) * dims, vmem_limit_bytes=VMEM_LIMIT
    )


def cost(flops, nbytes, exps=0):
    return pl.CostEstimate(flops=flops, bytes_accessed=nbytes, transcendentals=exps)


def row_block(width):
    return pl.BlockSpec((ROWS, width), lambda b, *_: (b, 0))


def block_live(lens_ref, length_all):
    per_seq = length_all // ROWS
    b = pl.program_id(0)
    return (b % per_seq) * ROWS < lens_ref[b // per_seq]


def norms_kernel(tokens_ref, affine_ref, normed_ref, mixed_ref):
    values = tokens_ref[...].astype(F32)
    centred = values - jnp.mean(values, axis=-1, keepdims=True)
    unit = centred * lax.rsqrt(jnp.mean(centred * centred, axis=-1, keepdims=True) + 1e-05)
    normed_ref[...] = (unit * affine_ref[0:1, :] + affine_ref[1:2, :]).astype(LOW)
    mixed_ref[...] = (unit * affine_ref[2:3, :] + affine_ref[3:4, :]).astype(LOW)


def both_norms(tokens, affine):
    rows, width = tokens.shape
    out = jax.ShapeDtypeStruct((rows, width), LOW)
    spec = pl.BlockSpec((256, width), lambda b: (b, 0))
    return pl.pallas_call(
        norms_kernel,
        grid=(rows // 256,),
        in_specs=[spec, whole((8, width))],
        out_specs=[spec, spec],
        out_shape=[out, out],
        compiler_params=params(),
        cost_estimate=cost(20 * rows * width, 6 * rows * width),
        name="both_norms",
    )(tokens, affine)


def turn_forward(values, cosine, after, before):
    part = values[:, :128]
    part = part * cosine + pltpu.roll(part, 32, 1) * after + pltpu.roll(part, 96, 1) * before
    return jnp.concatenate([part, values[:, 128:]], axis=1)


def turn_back(grad, cosine, after, before):
    part = grad[:, :128]
    part = part * cosine - pltpu.roll(part, 96, 1) * before - pltpu.roll(part, 32, 1) * after
    return jnp.concatenate([part, grad[:, 128:]], axis=1)


def attention_kernel(
    lens_ref,
    joint_ref,
    grad_ref,
    cos_ref,
    after_ref,
    before_ref,
    attended_ref,
    grad_joint_ref,
    bias_ref,
    query_s,
    key_s,
    value_s,
    grad_key_s,
    grad_value_s,
):
    seq = pl.program_id(0)
    length = lens_ref[seq]
    length_all = joint_ref.shape[0]
    tile = 256
    scale = HEAD ** (-0.5)
    grad_key_s[...] = jnp.zeros_like(grad_key_s)
    grad_value_s[...] = jnp.zeros_like(grad_value_s)

    @pl.when(seq == 0)
    def _():
        bias_ref[...] = jnp.zeros_like(bias_ref)

    for start in range(0, length_all, tile):
        rows = slice(start, start + tile)
        tables = (cos_ref[rows, :], after_ref[rows, :], before_ref[rows, :])
        query_s[rows, :] = turn_forward(joint_ref[rows, :HEAD], *tables).astype(LOW)
        key_s[rows, :] = turn_forward(joint_ref[rows, HEAD : 2 * HEAD], *tables).astype(LOW)
        value_s[rows, :] = joint_ref[rows, 2 * HEAD :].astype(LOW)

    for start in range(0, length_all, tile):
        rows = slice(start, start + tile)
        extent = start + tile

        @pl.when(start < length)
        def _(rows=rows, extent=extent, start=start):
            query = query_s[rows, :]
            keys = key_s[:extent, :]
            values = value_s[:extent, :]
            grad = grad_ref[rows, :]
            scores = dot_nt(query, keys) * scale
            row_id = start + lax.broadcasted_iota(jnp.int32, scores.shape, 0)
            column_id = lax.broadcasted_iota(jnp.int32, scores.shape, 1)
            allowed = (column_id <= row_id) & (column_id < length)
            scores = jnp.where(allowed, scores, -1e30)
            weights = jnp.exp(scores - jnp.max(scores, axis=-1, keepdims=True))
            probs = weights / jnp.sum(weights, axis=-1, keepdims=True)
            probs_low = probs.astype(LOW)
            attended_ref[rows, :] = dot_nn(probs_low, values).astype(LOW)
            grad_probs = dot_nt(grad, values)
            delta = jnp.sum(probs * grad_probs, axis=-1, keepdims=True)
            grad_scores = (probs * (grad_probs - delta)).astype(LOW)
            tables = (cos_ref[rows, :], after_ref[rows, :], before_ref[rows, :])
            grad_query = turn_back(dot_nn(grad_scores, keys) * scale, *tables).astype(LOW)
            grad_joint_ref[rows, :HEAD] = grad_query
            grad_key_s[:extent, :] += dot_tn(grad_scores, query)
            grad_value_s[:extent, :] += dot_tn(probs_low, grad)
            bias_ref[0:1, :HEAD] += jnp.sum(grad_query.astype(F32), axis=0, keepdims=True)

        @pl.when(start >= length)
        def _(rows=rows):
            attended_ref[rows, :] = jnp.zeros((tile, HEAD), LOW)
            grad_joint_ref[rows, :HEAD] = jnp.zeros((tile, HEAD), LOW)

    for start in range(0, length_all, tile):
        rows = slice(start, start + tile)
        tables = (cos_ref[rows, :], after_ref[rows, :], before_ref[rows, :])
        grad_key = turn_back(grad_key_s[rows, :] * scale, *tables).astype(LOW)
        grad_value = grad_value_s[rows, :].astype(LOW)
        grad_joint_ref[rows, HEAD : 2 * HEAD] = grad_key
        grad_joint_ref[rows, 2 * HEAD :] = grad_value
        bias_ref[0:1, HEAD : 2 * HEAD] += jnp.sum(grad_key.astype(F32), axis=0, keepdims=True)
        bias_ref[0:1, 2 * HEAD :] += jnp.sum(grad_value.astype(F32), axis=0, keepdims=True)


def attention_both(lens, joint, grad_attended, tables, length_all):
    rows = joint.shape[0]
    seqs = rows // length_all

    def per_seq(width):
        return pl.BlockSpec((length_all, width), lambda s, *_: (s, 0))

    return pl.pallas_call(
        attention_kernel,
        grid_spec=pltpu.PrefetchScalarGridSpec(
            num_scalar_prefetch=1,
            grid=(seqs,),
            in_specs=[per_seq(3 * HEAD), per_seq(HEAD)] + [whole((length_all, 128))] * 3,
            out_specs=[per_seq(HEAD), per_seq(3 * HEAD), whole((8, 3 * HEAD))],
            scratch_shapes=[pltpu.VMEM((length_all, HEAD), LOW)] * 3
            + [pltpu.VMEM((length_all, HEAD), F32)] * 2,
        ),
        out_shape=[
            jax.ShapeDtypeStruct((rows, HEAD), LOW),
            jax.ShapeDtypeStruct((rows, 3 * HEAD), LOW),
            jax.ShapeDtypeStruct((8, 3 * HEAD), F32),
        ],
        compiler_params=params(),
        cost_estimate=cost(12 * rows * length_all * HEAD, 14 * rows * HEAD, rows * length_all),
        name="attention_both",
    )(lens, joint, grad_attended, *tables)


def feed_kernel(length_all, pieces, lens_ref, *refs):
    mixed_ref, grad_ref, bias_ref = refs[:3]
    piece_refs = refs[3 : 3 + pieces]
    active_ref, grad_hidden_ref, bias_grad_ref = refs[3 + pieces : 6 + pieces]
    out_refs = refs[6 + pieces : 6 + 2 * pieces]
    up_s, down_s, up_acc, down_acc = refs[6 + 2 * pieces :]
    b = pl.program_id(0)

    @pl.when(b == 0)
    def _():
        at = 0
        for ref in piece_refs:
            for half in range(ref.shape[0]):
                up_s[at : at + 128, :] = ref[half, 0]
                down_s[at : at + 128, :] = ref[half, 1]
                at += 128
        up_acc[...] = jnp.zeros_like(up_acc)
        down_acc[...] = jnp.zeros_like(down_acc)
        bias_grad_ref[...] = jnp.zeros_like(bias_grad_ref)

    live = block_live(lens_ref, length_all)

    @pl.when(live)
    def _():
        mixed = mixed_ref[...]
        grad = grad_ref[...]
        hidden = dot_nt(mixed, up_s[...]) + bias_ref[0:1, :]
        gate = 0.5 * (1.0 + lax.erf(hidden * (2.0**-0.5)))
        active = (hidden * gate).astype(LOW)
        slope = gate + hidden * jnp.exp(-0.5 * hidden * hidden) * 0.3989422804014327
        grad_hidden32 = dot_nt(grad, down_s[...]) * slope
        grad_hidden = grad_hidden32.astype(LOW)
        active_ref[...] = active
        grad_hidden_ref[...] = grad_hidden
        bias_grad_ref[0:1, :] += jnp.sum(grad_hidden.astype(F32), axis=0, keepdims=True)
        down_acc[...] += dot_tn(active, grad)
        up_acc[...] += dot_tn(grad_hidden, mixed)

    @pl.when(jnp.logical_not(live))
    def _():
        active_ref[...] = jnp.zeros_like(active_ref)
        grad_hidden_ref[...] = jnp.zeros_like(grad_hidden_ref)

    @pl.when(b == pl.num_programs(0) - 1)
    def _():
        at = 0
        for ref in out_refs:
            for half in range(ref.shape[0]):
                ref[half, 0] = up_acc[at : at + 128, :].astype(LOW)
                ref[half, 1] = down_acc[at : at + 128, :].astype(LOW)
                at += 128


def feed_part(lens, mixed, grad_out, bias, pieces, length_all, name):
    rows, width = mixed.shape
    units = sum(128 * piece.shape[0] for piece in pieces)
    out = pl.pallas_call(
        partial(feed_kernel, length_all, len(pieces)),
        grid_spec=pltpu.PrefetchScalarGridSpec(
            num_scalar_prefetch=1,
            grid=(rows // ROWS,),
            in_specs=[row_block(width), row_block(width), whole((8, units))]
            + [whole(piece.shape) for piece in pieces],
            out_specs=[row_block(units), row_block(units), whole((8, units))]
            + [whole(piece.shape) for piece in pieces],
            scratch_shapes=[pltpu.VMEM((units, width), LOW)] * 2
            + [pltpu.VMEM((units, width), F32)] * 2,
        ),
        out_shape=[
            jax.ShapeDtypeStruct((rows, units), LOW),
            jax.ShapeDtypeStruct((rows, units), LOW),
            jax.ShapeDtypeStruct((8, units), F32),
        ]
        + [jax.ShapeDtypeStruct(piece.shape, LOW) for piece in pieces],
        compiler_params=params(),
        cost_estimate=cost(
            8 * rows * width * units, 4 * rows * width + 8 * units * width, 2 * rows * units
        ),
        name=name,
    )(lens, mixed, grad_out, jnp.broadcast_to(bias.astype(F32)[None, :], (8, units)), *pieces)
    return out[0], out[1], out[2][0], out[3:]


def output_kernel(length_all, parts, pieces, lens_ref, *refs):
    active_refs = refs[:parts]
    attended_ref, dense_ref = refs[parts : parts + 2]
    piece_refs = refs[parts + 2 : parts + 2 + pieces]
    out_ref, down_s = refs[parts + 2 + pieces :]

    @pl.when(pl.program_id(0) == 0)
    def _():
        at = 0
        for ref in piece_refs:
            for half in range(ref.shape[0]):
                down_s[at : at + 128, :] = ref[half, 1]
                at += 128

    live = block_live(lens_ref, length_all)

    @pl.when(live)
    def _():
        total = dot_nn(attended_ref[...], dense_ref[...])
        at = 0
        for ref in active_refs:
            total += dot_nn(ref[...], down_s[at : at + ref.shape[1], :])
            at += ref.shape[1]
        out_ref[...] = total.astype(LOW)

    @pl.when(jnp.logical_not(live))
    def _():
        out_ref[...] = jnp.zeros_like(out_ref)


def branch_output(lens, actives, attended, dense, pieces, length_all):
    rows, width = attended.shape[0], dense.shape[1]
    units = sum(active.shape[1] for active in actives)
    return pl.pallas_call(
        partial(output_kernel, length_all, len(actives), len(pieces)),
        grid_spec=pltpu.PrefetchScalarGridSpec(
            num_scalar_prefetch=1,
            grid=(rows // ROWS,),
            in_specs=[row_block(active.shape[1]) for active in actives]
            + [row_block(HEAD), whole(dense.shape)]
            + [whole(piece.shape) for piece in pieces],
            out_specs=row_block(width),
            scratch_shapes=[pltpu.VMEM((units, width), LOW)],
        ),
        out_shape=jax.ShapeDtypeStruct((rows, width), LOW),
        compiler_params=params(),
        cost_estimate=cost(
            2 * rows * width * (units + HEAD), 2 * rows * (width + units) + 4 * units * width
        ),
        name="branch_output",
    )(lens, *actives, attended, dense, *pieces)


def input_grad_kernel(length_all, parts, pieces, lens_ref, *refs):
    grad_refs = refs[:parts]
    grad_joint_ref, tokens_ref, affine_ref, qkv_ref = refs[parts : parts + 4]
    piece_refs = refs[parts + 4 : parts + 4 + pieces]
    out_ref, norm_ref, up_s = refs[parts + 4 + pieces :]
    b = pl.program_id(0)

    @pl.when(b == 0)
    def _():
        at = 0
        for ref in piece_refs:
            for half in range(ref.shape[0]):
                up_s[at : at + 128, :] = ref[half, 0]
                at += 128
        norm_ref[...] = jnp.zeros_like(norm_ref)

    live = block_live(lens_ref, length_all)

    @pl.when(live)
    def _():
        grad_one = dot_nn(grad_joint_ref[...], qkv_ref[...])
        grad_two = None
        at = 0
        for ref in grad_refs:
            term = dot_nn(ref[...], up_s[at : at + ref.shape[1], :])
            grad_two = term if grad_two is None else grad_two + term
            at += ref.shape[1]
        values = tokens_ref[...].astype(F32)
        centred = values - jnp.mean(values, axis=-1, keepdims=True)
        inverse = lax.rsqrt(jnp.mean(centred * centred, axis=-1, keepdims=True) + 1e-05)
        unit = centred * inverse
        norm_ref[0:1, :] += jnp.sum(grad_one * unit, axis=0, keepdims=True)
        norm_ref[1:2, :] += jnp.sum(grad_one, axis=0, keepdims=True)
        norm_ref[2:3, :] += jnp.sum(grad_two * unit, axis=0, keepdims=True)
        norm_ref[3:4, :] += jnp.sum(grad_two, axis=0, keepdims=True)
        scaled = grad_one * affine_ref[0:1, :] + grad_two * affine_ref[2:3, :]
        scaled_mean = jnp.mean(scaled, axis=-1, keepdims=True)
        along = jnp.mean(scaled * unit, axis=-1, keepdims=True)
        out_ref[...] = (inverse * (scaled - scaled_mean - unit * along)).astype(LOW)

    @pl.when(jnp.logical_not(live))
    def _():
        out_ref[...] = jnp.zeros_like(out_ref)


def input_grad_part(lens, grads, grad_joint, tokens, affine, qkv, pieces, length_all):
    rows, width = tokens.shape
    units = sum(grad.shape[1] for grad in grads)
    return pl.pallas_call(
        partial(input_grad_kernel, length_all, len(grads), len(pieces)),
        grid_spec=pltpu.PrefetchScalarGridSpec(
            num_scalar_prefetch=1,
            grid=(rows // ROWS,),
            in_specs=[row_block(grad.shape[1]) for grad in grads]
            + [row_block(3 * HEAD), row_block(width), whole((8, width)), whole(qkv.shape)]
            + [whole(piece.shape) for piece in pieces],
            out_specs=[row_block(width), whole((8, width))],
            scratch_shapes=[pltpu.VMEM((units, width), LOW)],
        ),
        out_shape=[
            jax.ShapeDtypeStruct((rows, width), LOW),
            jax.ShapeDtypeStruct((8, width), F32),
        ],
        compiler_params=params(),
        cost_estimate=cost(
            2 * rows * width * (units + 3 * HEAD), 4 * rows * (width + units) + 4 * units * width
        ),
        name="input_grad_part",
    )(lens, *grads, grad_joint, tokens, affine, qkv, *pieces)


def swap(value, bit):
    size = lax.axis_size("dp")
    return lax.ppermute(value, "dp", [(k, k ^ bit) for k in range(size)])


def add_low(*terms):
    total = terms[0].astype(F32)
    for term in terms[1:]:
        total = total + term.astype(F32)
    return total


def chain_scatter(partial_sum):
    size = lax.axis_size("tensor")
    here = lax.axis_index("tensor")
    part = partial_sum.shape[1] // size

    def columns(index):
        return lax.dynamic_slice_in_dim(partial_sum, index * part, part, 1)

    arrived = []
    for step, place in ((1, here), (-1, size - 1 - here)):
        carried = None
        for turn in range(1, size):
            index = jnp.clip(size - turn + place, 0, size - 1)
            index = index if step == 1 else size - 1 - index
            piece = columns(index)
            if carried is not None:
                piece = add_low(piece, carried).astype(LOW)
            pairs = []
            for source in range(min(turn, size - 1)):
                pair = (source, source + 1)
                pairs.append(pair if step == 1 else (size - 1 - pair[0], size - 1 - pair[1]))
            carried = lax.ppermute(piece, "tensor", pairs)
        arrived.append(carried)
    return add_low(columns(here), *arrived)


def small_scatter(value, axis, bits):
    place = lax.axis_index(axis)
    size = lax.axis_size(axis)
    for bit in bits:
        half = value.shape[0] // 2
        upper = (place // bit) % 2
        mine = lax.dynamic_slice_in_dim(value, upper * half, half, 0)
        theirs = lax.dynamic_slice_in_dim(value, (1 - upper) * half, half, 0)
        value = mine + lax.ppermute(theirs, axis, [(k, k ^ bit) for k in range(size)])
    return value[0]


def local_fast(
    tokens,
    cotangent,
    lengths,
    keep,
    first_gain,
    first_shift,
    second_gain,
    second_shift,
    qkv_weight,
    qkv_bias,
    dense_weight,
    up_weight,
    up_bias,
    down_weight,
    branch_bias,
):
    tokens, cotangent, keep = tokens[0], cotangent[0], keep[0]
    length_all, width = tokens.shape
    place = lax.axis_index("dp")
    core, chip = place % 2, place // 2
    dp_size, tensor_size = lax.axis_size("dp"), lax.axis_size("tensor")
    qkv_rows, dense_rows, units = qkv_weight.shape[1], dense_weight.shape[1], up_weight.shape[0]
    positions = jnp.arange(length_all)
    live = positions < lengths[0]
    affine = jnp.stack([first_gain, first_shift, second_gain, second_shift] * 2)

    mine = jnp.concatenate(
        [
            lax.dynamic_index_in_dim(qkv_weight, core, 0, False),
            lax.dynamic_index_in_dim(dense_weight, core, 0, False),
        ],
        axis=0,
    )
    theirs = jnp.concatenate(
        [
            lax.dynamic_index_in_dim(qkv_weight, 1 - core, 0, False),
            lax.dynamic_index_in_dim(dense_weight, 1 - core, 0, False),
        ],
        axis=0,
    )
    theirs = swap(theirs, 1)
    lower = jnp.where(core == 0, mine, theirs)
    upper = jnp.where(core == 0, theirs, mine)
    head_block = jnp.concatenate(
        [lower[:qkv_rows], upper[:qkv_rows], lower[qkv_rows:], upper[qkv_rows:]], axis=0
    )
    block_rows = head_block.shape[0]
    head_x, head_y = swap(head_block, 2), swap(head_block, 4)
    middle = block_rows // 2
    head_d = (swap(head_y[:middle], 2), swap(head_x[middle:], 4))

    feed_own = jnp.stack(
        [up_weight.reshape(2, units // 2, width), down_weight.reshape(2, units // 2, width)], axis=1
    )
    feed_own, head_x, head_y = lax.optimization_barrier((feed_own, head_x, head_y))
    feed_x, feed_y = swap(feed_own, 2), swap(feed_own, 4)
    feed_d = (swap(feed_y[:1], 2), swap(feed_x[1:], 4))

    grad_own = jnp.where((live & (keep == 1))[:, None], cotangent, jnp.zeros((), LOW))
    both_tokens = jnp.concatenate([tokens, swap(tokens, 1)], axis=0)
    grad_out = jnp.concatenate([grad_own, swap(grad_own, 1)], axis=0)
    lens = jnp.concatenate([lengths, swap(lengths, 1)])
    biases = jnp.concatenate([up_bias, qkv_bias.reshape(-1)])
    pad = -biases.shape[0] % 128
    biases = jnp.pad(biases, (0, pad))[None]
    for bit in (1, 2, 4):
        biases = jnp.concatenate([biases, swap(biases, bit)], axis=0)
    up_biases = biases[:, :units]
    qkv_biases = biases[:, units : units + 2 * qkv_rows].reshape(dp_size, 2, qkv_rows)
    qkv_biases = lax.dynamic_index_in_dim(qkv_biases, core, 1, False)
    qkv_bias_head = qkv_biases[place ^ jnp.arange(dp_size)].reshape(-1)

    normed, mixed = both_norms(both_tokens, affine)

    def feed(pieces, bits, name):
        bias = jnp.concatenate([up_biases[bit] for bit in bits])
        return feed_part(lens, mixed, grad_out, bias, pieces, length_all, name)

    active_a, grad_hidden_a, bias_a, (grad_feed_own,) = feed([feed_own], (0,), "feed_own")

    slots = (head_block, head_x, head_y, jnp.concatenate(head_d, axis=0))
    chip_qkv = 2 * qkv_rows
    qkv_full = jnp.zeros((4, chip_qkv, width), LOW)
    dense_full = jnp.zeros((4, block_rows - chip_qkv, width), LOW)
    for bits, slot in enumerate(slots):
        at = chip ^ bits
        qkv_full = lax.dynamic_update_index_in_dim(qkv_full, slot[:chip_qkv], at, 0)
        dense_full = lax.dynamic_update_index_in_dim(dense_full, slot[chip_qkv:], at, 0)
    qkv_full = qkv_full.reshape(4 * chip_qkv, width)
    dense_full = dense_full.reshape(-1, width)
    joint = dot_nt(normed, qkv_full) + qkv_bias_head.astype(F32)
    grad_attended = dot_nt(grad_out, dense_full).astype(LOW)
    cosine, sine = rotary_tables(0, length_all)
    cosine, sine = cosine[:, 0], sine[:, 0]
    half = ROT // 2
    zeros = jnp.zeros((length_all, 128 - ROT), F32)
    blank = jnp.zeros((length_all, half), F32)
    tables = (
        jnp.concatenate([cosine, zeros + 1.0], axis=1),
        jnp.concatenate([blank, sine[:, half:], zeros], axis=1),
        jnp.concatenate([-sine[:, :half], blank, zeros], axis=1),
    )
    attended, grad_joint, bias_joint = attention_both(
        lens, joint, grad_attended, tables, length_all
    )
    grad_dense = dot_tn(attended, grad_out).astype(LOW)
    grad_qkv = dot_tn(grad_joint, normed).astype(LOW)

    active_b, grad_hidden_b, bias_b, (grad_feed_x, grad_feed_y) = feed(
        [feed_x, feed_y], (2, 4), "feed_neighbours"
    )
    active_c, grad_hidden_c, bias_c, grad_feed_d = feed(list(feed_d), (6,), "feed_far")
    pieces = [feed_own, feed_x, feed_y, *feed_d]
    branch = branch_output(
        lens, [active_a, active_b, active_c], attended, dense_full, pieces, length_all
    )
    branch_here = add_low(branch[:length_all], swap(branch[length_all:], 1)).astype(LOW)
    branch_total = chain_scatter(branch_here)
    slice_width = width // tensor_size
    column_start = lax.axis_index("tensor") * slice_width
    token_slice = lax.dynamic_slice_in_dim(tokens, column_start, slice_width, 1).astype(F32)
    bias_slice = lax.dynamic_slice_in_dim(branch_bias, column_start, slice_width, 0)
    block_out = (token_slice + jnp.where(live[:, None], branch_total + bias_slice, 0.0)).astype(LOW)

    grad_x, norm_sums = input_grad_part(
        lens,
        [grad_hidden_a, grad_hidden_b, grad_hidden_c],
        grad_joint,
        both_tokens,
        affine,
        qkv_full,
        pieces,
        length_all,
    )
    grad_x_here = add_low(grad_x[:length_all], swap(grad_x[length_all:], 1)).astype(LOW)
    grad_x_total = chain_scatter(grad_x_here)
    grad_slice = lax.dynamic_slice_in_dim(grad_own, column_start, slice_width, 1).astype(F32)
    input_grad = (grad_slice + grad_x_total).astype(LOW)

    def scatter(own, over_x, over_y, far):
        through_x, through_y = swap(far[0], 2), swap(far[1], 4)
        over_y = (add_low(over_y[0], through_x).astype(LOW), over_y[1])
        over_x = (over_x[0], add_low(over_x[1], through_y).astype(LOW))
        from_x = [swap(item, 2) for item in over_x]
        from_y = [swap(item, 4) for item in over_y]
        return [add_low(own[k], from_x[k], from_y[k]) for k in range(2)]

    def halves(value):
        return (value[0], value[1])

    feed_grad = scatter(
        halves(grad_feed_own),
        halves(grad_feed_x),
        halves(grad_feed_y),
        (grad_feed_d[0][0], grad_feed_d[1][0]),
    )
    up_grad_out = jnp.concatenate([item[0] for item in feed_grad], axis=0)
    down_grad_out = jnp.concatenate([item[1] for item in feed_grad], axis=0)

    def head_slot(bits):
        at = chip ^ bits
        block = jnp.concatenate(
            [
                lax.dynamic_slice_in_dim(grad_qkv, at * chip_qkv, chip_qkv, 0),
                lax.dynamic_slice_in_dim(
                    grad_dense, at * (block_rows - chip_qkv), block_rows - chip_qkv, 0
                ),
            ],
            axis=0,
        )
        return (block[:middle], block[middle:])

    head_grad = jnp.concatenate(scatter(*[head_slot(bits) for bits in range(4)]), axis=0)
    head_lower = jnp.concatenate(
        [head_grad[:qkv_rows], head_grad[chip_qkv : chip_qkv + dense_rows]], axis=0
    )
    head_upper = jnp.concatenate(
        [head_grad[qkv_rows:chip_qkv], head_grad[chip_qkv + dense_rows :]], axis=0
    )
    head_mine = jnp.where(core == 0, head_lower, head_upper)
    head_other = swap(jnp.where(core == 0, head_upper, head_lower).astype(LOW), 1).astype(F32)
    head_out = jnp.stack(
        [
            jnp.where(core == 0, head_mine, head_other),
            jnp.where(core == 0, head_other, head_mine),
        ]
    )
    qkv_grad_out, dense_grad_out = head_out[:, :qkv_rows], head_out[:, qkv_rows:]

    column_bias = jnp.stack(
        [bias_a, bias_b[:units], bias_b[units:], bias_c], axis=0
    )[chip ^ jnp.arange(4)]
    column_bias = jnp.stack(
        [jnp.where(core == 0, column_bias, 0.0), jnp.where(core == 0, 0.0, column_bias)], axis=1
    ).reshape(dp_size, units)
    head_bias = bias_joint[0].reshape(dp_size, qkv_rows)
    head_bias = jnp.concatenate(
        [jnp.where(core == 0, head_bias, 0.0), jnp.where(core == 0, 0.0, head_bias)], axis=1
    )
    row_width = length_all // tensor_size
    bias_term = jnp.sum(
        lax.dynamic_slice_in_dim(
            grad_own, lax.axis_index("tensor") * row_width, row_width, 0
        ).astype(F32),
        axis=0,
    )
    norm_rows = jnp.concatenate([norm_sums[:4], bias_term[None]], axis=0)
    norm_rows = norm_rows.reshape(5, dp_size, -1).transpose(1, 0, 2).reshape(dp_size, -1)
    small = jnp.concatenate([column_bias, head_bias, norm_rows], axis=1)
    small = jnp.pad(small, ((0, 0), (0, -small.shape[1] % 128)))
    small = small_scatter(small, "dp", (4, 2, 1))
    up_bias_grad_out = small[:units]
    qkv_bias_grad_out = small[units : units + 2 * qkv_rows].reshape(2, qkv_rows)
    at = units + 2 * qkv_rows
    norms = small[at : at + 5 * width // dp_size].reshape(5, tensor_size, -1).transpose(1, 0, 2)
    bits = [1 << k for k in reversed(range(tensor_size.bit_length() - 1))]
    norms_out = small_scatter(norms.reshape(tensor_size, -1), "tensor", bits).reshape(5, -1)
    return (
        block_out[None],
        input_grad[None],
        qkv_grad_out,
        qkv_bias_grad_out,
        dense_grad_out,
        up_grad_out,
        up_bias_grad_out,
        down_grad_out,
        norms_out,
    )


def solution(mesh):
    in_specs = (
        P("dp", None, None),
        P("dp", None, None),
        P("dp"),
        P("dp", None),
        P(),
        P(),
        P(),
        P(),
        P("tensor", "dp", None),
        P("tensor", "dp"),
        P("tensor", "dp", None),
        P(("dp", "tensor"), None),
        P(("dp", "tensor")),
        P(("dp", "tensor"), None),
        P(),
    )
    out_specs = (
        P("dp", None, "tensor"),
        P("dp", None, "tensor"),
        P("tensor", "dp", None),
        P("tensor", "dp"),
        P("tensor", "dp", None),
        P(("dp", "tensor"), None),
        P(("dp", "tensor")),
        P(("dp", "tensor"), None),
        P(None, ("dp", "tensor")),
    )

    def local(*items):
        heads_here = items[8].shape[0]
        fits = mesh.shape["dp"] == 8 and heads_here == 2 and items[0].shape[0] == 1
        return (local_fast if fits else local_general)(*items)

    return jax.shard_map(local, mesh=mesh, in_specs=in_specs, out_specs=out_specs, check_vma=False)
```

```python
from functools import partial

import jax
import jax.numpy as jnp
from jax import lax
from jax.experimental import pallas as pl
from jax.experimental.pallas import tpu as pltpu
from jax.sharding import PartitionSpec as P


HEADS = 8
HEAD = 256
ROT = 64
BLOCK = 512


def layer_norm_parts(values, gain, shift):
    centred = values - jnp.mean(values, axis=-1, keepdims=True)
    inverse = lax.rsqrt(jnp.mean(centred * centred, axis=-1, keepdims=True) + 1e-05)
    unit = centred * inverse
    return (unit * gain + shift, unit, inverse)


def norm_back(grad, unit, inverse, gain):
    scaled = grad * gain
    centred = scaled - jnp.mean(scaled, axis=-1, keepdims=True)
    return inverse * (centred - unit * jnp.mean(scaled * unit, axis=-1, keepdims=True))


def rotary_tables(start, count):
    half = ROT // 2
    inverse = 10000.0 ** (-jnp.arange(half, dtype=jnp.float32) * 2.0 / ROT)
    angles = (start + jnp.arange(count, dtype=jnp.float32))[:, None] * inverse[None, :]
    angles = jnp.concatenate([angles, angles], axis=1)
    return (jnp.cos(angles)[:, None, :], jnp.sin(angles)[:, None, :])


def rotate(values, cosine, sine):
    half = ROT // 2
    part = values[..., :ROT]
    turned = jnp.concatenate([-part[..., half:], part[..., :half]], axis=-1)
    return jnp.concatenate([part * cosine + turned * sine, values[..., ROT:]], axis=-1)


def rotate_back(grad, cosine, sine):
    half = ROT // 2
    part = grad[..., :ROT]
    scaled = part * sine
    turned = jnp.concatenate([scaled[..., half:], -scaled[..., :half]], axis=-1)
    return jnp.concatenate([part * cosine + turned, grad[..., ROT:]], axis=-1)


def block_scores(query_block, key_rows, query_start, key_start, length):
    scores = jnp.einsum(
        "qhe,khe->hqk", query_block, key_rows, preferred_element_type=jnp.float32
    ) * HEAD ** (-0.5)
    rows = query_start + jnp.arange(query_block.shape[0])
    columns = key_start + jnp.arange(key_rows.shape[0])
    allowed = (columns[None, :] <= rows[:, None]) & (columns[None, :] < length)
    return jnp.where(allowed[None], scores, -1e30)


def when_live(flag, work, operand):
    return lax.cond(flag, work, lambda unused: jax.tree.map(jnp.zeros_like, work(unused)), operand)


def local_general(
    tokens,
    cotangent,
    lengths,
    keep,
    first_gain,
    first_shift,
    second_gain,
    second_shift,
    qkv_weight,
    qkv_bias,
    dense_weight,
    up_weight,
    up_bias,
    down_weight,
    branch_bias,
):
    gathered = (
        lax.all_gather(qkv_weight, "dp", axis=1, tiled=True),
        lax.all_gather(qkv_bias, "dp", axis=1, tiled=True),
        lax.all_gather(dense_weight, "dp", axis=1, tiled=True),
        lax.all_gather(up_weight, "dp", axis=0, tiled=True),
        lax.all_gather(up_bias, "dp", axis=0, tiled=True),
        lax.all_gather(down_weight, "dp", axis=0, tiled=True),
    )
    qkv_full, qkv_bias_full, dense_full, up_full, up_bias_full, down_full = gathered
    _, length_all, width = tokens.shape
    blocks = length_all // BLOCK
    heads_here = qkv_full.shape[0]
    hidden_here = up_full.shape[0]
    scale = HEAD ** (-0.5)
    positions = jnp.arange(length_all)
    live_rows = positions[None, :] < lengths[:, None]

    def forward_one(items):
        row_tokens, length = items
        dense_flat = dense_full.reshape(heads_here * HEAD, width)

        def project(row_block, start):
            values32 = row_block.astype(jnp.float32)
            normed = layer_norm_parts(values32, first_gain, first_shift)[0].astype(jnp.bfloat16)
            joint = jnp.einsum(
                "bd,hed->bhe", normed, qkv_full, preferred_element_type=jnp.float32
            ) + qkv_bias_full.astype(jnp.float32)
            cosine, sine = rotary_tables(start, BLOCK)
            query_rows = rotate(joint[..., :HEAD], cosine, sine).astype(jnp.bfloat16)
            key_rows = rotate(joint[..., HEAD : 2 * HEAD], cosine, sine).astype(jnp.bfloat16)
            value_rows = joint[..., 2 * HEAD :].astype(jnp.bfloat16)
            mixed = layer_norm_parts(values32, second_gain, second_shift)[0].astype(jnp.bfloat16)
            hidden_rows = jnp.einsum(
                "bd,fd->bf", mixed, up_full, preferred_element_type=jnp.float32
            ) + up_bias_full.astype(jnp.float32)
            active = jax.nn.gelu(hidden_rows, approximate=False).astype(jnp.bfloat16)
            feed = jnp.dot(active, down_full, preferred_element_type=jnp.float32)
            return (query_rows, key_rows, value_rows, hidden_rows, feed)

        outputs = []
        for index in range(blocks):
            start = index * BLOCK
            outputs.append(
                when_live(
                    start < length, partial(project, start=start), row_tokens[start : start + BLOCK]
                )
            )
        query_all = jnp.concatenate([item[0] for item in outputs], axis=0)
        keys_all = jnp.concatenate([item[1] for item in outputs], axis=0)
        values_all = jnp.concatenate([item[2] for item in outputs], axis=0)
        hidden_all = jnp.concatenate([item[3] for item in outputs], axis=0)
        feed_all = jnp.concatenate([item[4] for item in outputs], axis=0)

        def attend(query_block, start):
            peak = jnp.full((heads_here, BLOCK, 1), -1e30, jnp.float32)
            total = jnp.zeros((heads_here, BLOCK, 1), jnp.float32)
            for key_index in range(start // BLOCK + 1):
                key_start = key_index * BLOCK
                scores = block_scores(
                    query_block, keys_all[key_start : key_start + BLOCK], start, key_start, length
                )
                newer = jnp.maximum(peak, jnp.max(scores, axis=-1, keepdims=True))
                total = total * jnp.exp(peak - newer) + jnp.sum(
                    jnp.exp(scores - newer), axis=-1, keepdims=True
                )
                peak = newer
            logsum = peak + jnp.log(total)
            summed = jnp.zeros((BLOCK, heads_here, HEAD), jnp.float32)
            for key_index in range(start // BLOCK + 1):
                key_start = key_index * BLOCK
                scores = block_scores(
                    query_block, keys_all[key_start : key_start + BLOCK], start, key_start, length
                )
                probs = jnp.exp(scores - logsum).astype(jnp.bfloat16)
                summed = summed + jnp.einsum(
                    "hqk,khe->qhe",
                    probs,
                    values_all[key_start : key_start + BLOCK],
                    preferred_element_type=jnp.float32,
                )
            attended_block = summed.astype(jnp.bfloat16).reshape(BLOCK, heads_here * HEAD)
            attention_rows = jnp.dot(attended_block, dense_flat, preferred_element_type=jnp.float32)
            return (attended_block, logsum[..., 0], attention_rows)

        pieces = []
        for index in range(blocks):
            start = index * BLOCK
            pieces.append(
                when_live(
                    start < length, partial(attend, start=start), query_all[start : start + BLOCK]
                )
            )
        attended_all = jnp.concatenate([item[0] for item in pieces], axis=0)
        logsum_all = jnp.concatenate([item[1] for item in pieces], axis=1)
        attention_all = jnp.concatenate([item[2] for item in pieces], axis=0)
        live = (positions < length)[:, None]
        branch_part = jnp.where(live, attention_all + feed_all, 0.0)
        return (branch_part, query_all, keys_all, values_all, hidden_all, attended_all, logsum_all)

    branch_part, query_all, keys_all, values_all, hidden_all, attended_all, logsum_all = lax.map(
        forward_one, (tokens, lengths)
    )
    branch_total = lax.psum_scatter(branch_part, "tensor", scatter_dimension=2, tiled=True)
    slice_width = branch_total.shape[2]
    column_start = lax.axis_index("tensor") * slice_width
    token_slice = lax.dynamic_slice_in_dim(tokens, column_start, slice_width, 2).astype(jnp.float32)
    bias_slice = lax.dynamic_slice_in_dim(branch_bias, column_start, slice_width, 0)
    block_out = (
        token_slice + jnp.where(live_rows[..., None], branch_total + bias_slice, 0.0)
    ).astype(jnp.bfloat16)
    qkv_back, dense_back, up_back, down_back = (
        lax.all_gather(qkv_weight, "dp", axis=1, tiled=True),
        lax.all_gather(dense_weight, "dp", axis=1, tiled=True),
        lax.all_gather(up_weight, "dp", axis=0, tiled=True),
        lax.all_gather(down_weight, "dp", axis=0, tiled=True),
    )
    dense_back_flat = dense_back.reshape(heads_here * HEAD, width)
    valid = live_rows & (keep == 1)
    grad_out = jnp.where(valid[..., None], cotangent, jnp.zeros((), jnp.bfloat16))
    row_width = length_all // lax.axis_size("tensor")
    row_start = lax.axis_index("tensor") * row_width
    bias_term = jnp.sum(
        lax.dynamic_slice_in_dim(grad_out, row_start, row_width, 1).astype(jnp.float32), axis=(0, 1)
    )

    def feed_back(carry, items):
        row_tokens, row_grad, row_hidden, length = items
        outputs = []
        for index in range(blocks):
            start = index * BLOCK

            def work(operand, start=start):
                grad_up, grad_up_bias, grad_down, gain_two, shift_two = operand
                values32 = row_tokens[start : start + BLOCK].astype(jnp.float32)
                normed, unit, inverse = layer_norm_parts(values32, second_gain, second_shift)
                mixed = normed.astype(jnp.bfloat16)
                grad_rows = row_grad[start : start + BLOCK]
                hidden_rows = row_hidden[start : start + BLOCK]
                grad_active = jnp.einsum(
                    "bd,fd->bf", grad_rows, down_back, preferred_element_type=jnp.float32
                )
                active, gelu_back = jax.vjp(partial(jax.nn.gelu, approximate=False), hidden_rows)
                grad_hidden = gelu_back(grad_active)[0].astype(jnp.bfloat16)
                grad_down = grad_down + jnp.einsum(
                    "bf,bd->fd",
                    active.astype(jnp.bfloat16),
                    grad_rows,
                    preferred_element_type=jnp.float32,
                )
                grad_up = grad_up + jnp.einsum(
                    "bf,bd->fd", grad_hidden, mixed, preferred_element_type=jnp.float32
                )
                grad_up_bias = grad_up_bias + jnp.sum(grad_hidden.astype(jnp.float32), axis=0)
                grad_mixed = jnp.dot(grad_hidden, up_back, preferred_element_type=jnp.float32)
                gain_two = gain_two + jnp.sum(grad_mixed * unit, axis=0)
                shift_two = shift_two + jnp.sum(grad_mixed, axis=0)
                return (
                    (grad_up, grad_up_bias, grad_down, gain_two, shift_two),
                    norm_back(grad_mixed, unit, inverse, second_gain),
                )

            carry, piece = lax.cond(
                start < length,
                work,
                lambda operand: (operand, jnp.zeros((BLOCK, width), jnp.float32)),
                carry,
            )
            outputs.append(piece)
        return (carry, jnp.concatenate(outputs, axis=0))

    feed_init = (
        jnp.zeros((hidden_here, width), jnp.float32),
        jnp.zeros((hidden_here,), jnp.float32),
        jnp.zeros((hidden_here, width), jnp.float32),
        jnp.zeros((width,), jnp.float32),
        jnp.zeros((width,), jnp.float32),
    )
    feed_totals, grad_x_two = lax.scan(
        feed_back, feed_init, (tokens, grad_out, hidden_all, lengths)
    )
    grad_up_total, grad_up_bias_total, grad_down_total, gain_two, shift_two = feed_totals

    def attention_back(carry, items):
        (
            row_tokens,
            row_grad,
            query_rows,
            key_rows,
            value_rows,
            attended_rows,
            logsum_rows,
            length,
        ) = items
        grad_qkv, grad_qkv_bias, grad_dense, gain_one, shift_one = carry
        grad_attended = jnp.einsum(
            "ld,nd->ln", row_grad, dense_back_flat, preferred_element_type=jnp.float32
        ).astype(jnp.bfloat16)
        grad_dense = grad_dense + jnp.einsum(
            "ln,ld->nd", attended_rows, row_grad, preferred_element_type=jnp.float32
        )
        grad_attended = grad_attended.reshape(length_all, heads_here, HEAD)
        grad_keys = jnp.zeros((length_all, heads_here, HEAD), jnp.float32)
        grad_values = jnp.zeros((length_all, heads_here, HEAD), jnp.float32)
        query_grads = []
        for query_index in range(blocks):
            query_start = query_index * BLOCK

            def work(operand, query_start=query_start, query_index=query_index):
                grad_keys_now, grad_values_now = operand
                query_block = query_rows[query_start : query_start + BLOCK]
                grad_block = grad_attended[query_start : query_start + BLOCK]
                logsum_block = logsum_rows[:, query_start : query_start + BLOCK][..., None]

                def probs_and_grad(key_start):
                    scores = block_scores(
                        query_block,
                        key_rows[key_start : key_start + BLOCK],
                        query_start,
                        key_start,
                        length,
                    )
                    probs = jnp.exp(scores - logsum_block)
                    grad_probs = jnp.einsum(
                        "qhe,khe->hqk",
                        grad_block,
                        value_rows[key_start : key_start + BLOCK],
                        preferred_element_type=jnp.float32,
                    )
                    return (probs, grad_probs)

                delta = jnp.zeros((heads_here, BLOCK, 1), jnp.float32)
                for key_index in range(query_index + 1):
                    probs, grad_probs = probs_and_grad(key_index * BLOCK)
                    delta = delta + jnp.sum(probs * grad_probs, axis=-1, keepdims=True)
                grad_query_block = jnp.zeros((BLOCK, heads_here, HEAD), jnp.float32)
                for key_index in range(query_index + 1):
                    key_start = key_index * BLOCK
                    probs, grad_probs = probs_and_grad(key_start)
                    grad_scores = (probs * (grad_probs - delta)).astype(jnp.bfloat16)
                    grad_query_block = (
                        grad_query_block
                        + jnp.einsum(
                            "hqk,khe->qhe",
                            grad_scores,
                            key_rows[key_start : key_start + BLOCK],
                            preferred_element_type=jnp.float32,
                        )
                        * scale
                    )
                    grad_keys_now = grad_keys_now.at[key_start : key_start + BLOCK].add(
                        jnp.einsum(
                            "hqk,qhe->khe",
                            grad_scores,
                            query_block,
                            preferred_element_type=jnp.float32,
                        )
                        * scale
                    )
                    grad_values_now = grad_values_now.at[key_start : key_start + BLOCK].add(
                        jnp.einsum(
                            "hqk,qhe->khe",
                            probs.astype(jnp.bfloat16),
                            grad_block,
                            preferred_element_type=jnp.float32,
                        )
                    )
                return ((grad_keys_now, grad_values_now), grad_query_block)

            (grad_keys, grad_values), query_piece = lax.cond(
                query_start < length,
                work,
                lambda operand: (operand, jnp.zeros((BLOCK, heads_here, HEAD), jnp.float32)),
                (grad_keys, grad_values),
            )
            query_grads.append(query_piece)
        grad_query = jnp.concatenate(query_grads, axis=0)
        cosine, sine = rotary_tables(0, length_all)
        grad_joint = jnp.concatenate(
            [
                rotate_back(grad_query, cosine, sine),
                rotate_back(grad_keys, cosine, sine),
                grad_values,
            ],
            axis=-1,
        ).astype(jnp.bfloat16)
        inner = (grad_qkv, grad_qkv_bias, gain_one, shift_one)
        outputs = []
        for index in range(blocks):
            start = index * BLOCK

            def work_norm(operand, start=start):
                grad_qkv_now, grad_bias_now, gain_now, shift_now = operand
                values32 = row_tokens[start : start + BLOCK].astype(jnp.float32)
                normed, unit, inverse = layer_norm_parts(values32, first_gain, first_shift)
                grad_rows = grad_joint[start : start + BLOCK]
                grad_qkv_now = grad_qkv_now + jnp.einsum(
                    "bhe,bd->hed",
                    grad_rows,
                    normed.astype(jnp.bfloat16),
                    preferred_element_type=jnp.float32,
                )
                grad_bias_now = grad_bias_now + jnp.sum(grad_rows.astype(jnp.float32), axis=0)
                grad_normed = jnp.einsum(
                    "bhe,hed->bd", grad_rows, qkv_back, preferred_element_type=jnp.float32
                )
                gain_now = gain_now + jnp.sum(grad_normed * unit, axis=0)
                shift_now = shift_now + jnp.sum(grad_normed, axis=0)
                return (
                    (grad_qkv_now, grad_bias_now, gain_now, shift_now),
                    norm_back(grad_normed, unit, inverse, first_gain),
                )

            inner, piece = lax.cond(
                start < length,
                work_norm,
                lambda operand: (operand, jnp.zeros((BLOCK, width), jnp.float32)),
                inner,
            )
            outputs.append(piece)
        grad_qkv, grad_qkv_bias, gain_one, shift_one = inner
        return (
            (grad_qkv, grad_qkv_bias, grad_dense, gain_one, shift_one),
            jnp.concatenate(outputs, axis=0),
        )

    attention_init = (
        jnp.zeros(qkv_back.shape, jnp.float32),
        jnp.zeros((heads_here, 3 * HEAD), jnp.float32),
        jnp.zeros((heads_here * HEAD, width), jnp.float32),
        jnp.zeros((width,), jnp.float32),
        jnp.zeros((width,), jnp.float32),
    )
    attention_totals, grad_x_one = lax.scan(
        attention_back,
        attention_init,
        (tokens, grad_out, query_all, keys_all, values_all, attended_all, logsum_all, lengths),
    )
    grad_qkv_total, grad_qkv_bias_total, grad_dense_total, gain_one, shift_one = attention_totals
    grad_dense_total = grad_dense_total.reshape(heads_here, HEAD, width)
    norms_total = jnp.stack([gain_one, shift_one, gain_two, shift_two, bias_term])
    (
        qkv_grad_out,
        qkv_bias_grad_out,
        dense_grad_out,
        up_grad_out,
        up_bias_grad_out,
        down_grad_out,
        norms_dp,
    ) = (
        lax.psum_scatter(
            grad_qkv_total.astype(jnp.bfloat16), "dp", scatter_dimension=1, tiled=True
        ).astype(jnp.float32),
        lax.psum_scatter(
            grad_qkv_bias_total.astype(jnp.bfloat16), "dp", scatter_dimension=1, tiled=True
        ).astype(jnp.float32),
        lax.psum_scatter(
            grad_dense_total.astype(jnp.bfloat16), "dp", scatter_dimension=1, tiled=True
        ).astype(jnp.float32),
        lax.psum_scatter(
            grad_up_total.astype(jnp.bfloat16), "dp", scatter_dimension=0, tiled=True
        ).astype(jnp.float32),
        lax.psum_scatter(
            grad_up_bias_total.astype(jnp.bfloat16), "dp", scatter_dimension=0, tiled=True
        ).astype(jnp.float32),
        lax.psum_scatter(
            grad_down_total.astype(jnp.bfloat16), "dp", scatter_dimension=0, tiled=True
        ).astype(jnp.float32),
        lax.psum_scatter(
            norms_total.astype(jnp.bfloat16), "dp", scatter_dimension=1, tiled=True
        ).astype(jnp.float32),
    )
    grad_x_partial = grad_x_one + grad_x_two
    grad_x_total, norms_out = (
        lax.psum_scatter(grad_x_partial, "tensor", scatter_dimension=2, tiled=True),
        lax.psum_scatter(norms_dp, "tensor", scatter_dimension=1, tiled=True),
    )
    grad_slice = lax.dynamic_slice_in_dim(grad_out, column_start, slice_width, 2).astype(
        jnp.float32
    )
    input_grad = (grad_slice + grad_x_total).astype(jnp.bfloat16)
    return (
        block_out,
        input_grad,
        qkv_grad_out,
        qkv_bias_grad_out,
        dense_grad_out,
        up_grad_out,
        up_bias_grad_out,
        down_grad_out,
        norms_out,
    )


F32 = jnp.float32
LOW = jnp.bfloat16
ROWS = 512
PARTS = 4
VMEM_LIMIT = 60 * 1024 * 1024


def dot_nt(left, right):
    return lax.dot_general(left, right, (((1,), (1,)), ((), ())), preferred_element_type=F32)


def dot_nn(left, right):
    return lax.dot_general(left, right, (((1,), (0,)), ((), ())), preferred_element_type=F32)


def dot_tn(left, right):
    return lax.dot_general(left, right, (((0,), (0,)), ((), ())), preferred_element_type=F32)


def whole(shape):
    return pl.BlockSpec(shape, lambda *_: (0,) * len(shape), pipeline_mode=pl.Buffered(1))


def params(dims=1):
    return pltpu.CompilerParams(
        dimension_semantics=("arbitrary",) * dims, vmem_limit_bytes=VMEM_LIMIT
    )


def cost(flops, nbytes, exps=0):
    return pl.CostEstimate(flops=flops, bytes_accessed=nbytes, transcendentals=exps)


def row_block(width):
    return pl.BlockSpec((ROWS, width), lambda b, *_: (b, 0))


def block_live(lens_ref, length_all):
    per_seq = length_all // ROWS
    b = pl.program_id(0)
    return (b % per_seq) * ROWS < lens_ref[b // per_seq]


def seq_block(width, length_all, seq):
    return pl.BlockSpec((ROWS, width), lambda b, *_: (b + seq * (length_all // ROWS), 0))


def unit_rows(values):
    values = values.astype(F32)
    centred = values - jnp.mean(values, axis=-1, keepdims=True)
    inverse = lax.rsqrt(jnp.mean(centred * centred, axis=-1, keepdims=True) + 1e-05)
    return centred * inverse, inverse


def norms_kernel(tokens_ref, grad_ref, valid_ref, affine_ref, *refs):
    normed_ref, mixed_ref, out_ref = refs[-3:]

    unit, _ = unit_rows(tokens_ref[...])
    normed_ref[...] = (unit * affine_ref[0:1, :] + affine_ref[1:2, :]).astype(LOW)
    mixed_ref[...] = (unit * affine_ref[2:3, :] + affine_ref[3:4, :]).astype(LOW)
    out_ref[...] = (grad_ref[...].astype(F32) * valid_ref[...]).astype(LOW)


def both_norms(tokens, cotangent, valid, affine, into, index):
    rows, width = tokens.shape
    steps = rows // 256
    out = jax.ShapeDtypeStruct((2 * rows, width), LOW)
    spec = pl.BlockSpec((256, width), lambda b: (b, 0))
    return pl.pallas_call(
        norms_kernel,
        grid=(steps,),
        in_specs=[spec, spec, pl.BlockSpec((256, 1), lambda b: (b, 0)), whole((8, width))]
        + [pl.BlockSpec(memory_space=pl.ANY)] * len(into),
        out_specs=[pl.BlockSpec((256, width), lambda b: (b + index * steps, 0))] * 3,
        out_shape=[out] * 3,
        input_output_aliases={4 + k: k for k in range(len(into))},
        compiler_params=params(),
        cost_estimate=cost(20 * rows * width, 10 * rows * width),
    )(tokens, cotangent, valid, affine, *into)


def turn_forward(values, cosine, after, before):
    part = values[:, :128]
    part = part * cosine + pltpu.roll(part, 32, 1) * after + pltpu.roll(part, 96, 1) * before
    return jnp.concatenate([part, values[:, 128:]], axis=1)


def turn_back(grad, cosine, after, before):
    part = grad[:, :128]
    part = part * cosine - pltpu.roll(part, 96, 1) * before - pltpu.roll(part, 32, 1) * after
    return jnp.concatenate([part, grad[:, 128:]], axis=1)


SLABS = ((0, (0, 1)), (1, (0, 1)), (2, (0, 1)), (3, (0,)), (3, (1,)))
SINGLE_SLABS = tuple((bits, (slab,)) for bits in range(4) for slab in range(2))


def project_kernel(chip_ref, *refs):
    normed_ref, grad_ref, bias_ref, cos_ref, after_ref, before_ref = refs[:6]
    slot_refs = refs[6:11]
    query_ref, grad_attended_ref, weight_ref, dense_ref = refs[11:]
    chip = chip_ref[0]
    rows_of_head = weight_ref.shape[0] // 8
    rows_of_dense = dense_ref.shape[0] // 8

    @pl.when(pl.program_id(0) == 0)
    def _():
        for ref, (bits, slabs) in zip(slot_refs, SLABS):
            for k, slab in enumerate(slabs):
                at = jnp.bitwise_xor(chip, bits) * 2 + slab
                head_at = pl.multiple_of(at * rows_of_head, 32)
                dense_at = pl.multiple_of(at * rows_of_dense, 32)
                weight_ref[pl.ds(head_at, rows_of_head), :] = ref[k, :rows_of_head, :]
                dense_ref[pl.ds(dense_at, rows_of_dense), :] = ref[k, rows_of_head:, :]

    joint = dot_nt(normed_ref[...], weight_ref[...]) + bias_ref[0:1, :]
    tables = (cos_ref[...], after_ref[...], before_ref[...])
    query_ref[:, :HEAD] = turn_forward(joint[:, :HEAD], *tables).astype(LOW)
    query_ref[:, HEAD : 2 * HEAD] = turn_forward(joint[:, HEAD : 2 * HEAD], *tables).astype(LOW)
    query_ref[:, 2 * HEAD :] = joint[:, 2 * HEAD :].astype(LOW)
    grad_attended_ref[...] = dot_nt(grad_ref[...], dense_ref[...]).astype(LOW)


def project(chip, normed, grad_out, bias, tables, slots, length_all):
    rows, width = normed.shape
    per_seq = length_all // ROWS
    table = pl.BlockSpec((ROWS, 128), lambda b, *_: (b % per_seq, 0))
    shapes = [
        jax.ShapeDtypeStruct((rows, 3 * HEAD), LOW),
        jax.ShapeDtypeStruct((rows, HEAD), LOW),
        jax.ShapeDtypeStruct((3 * HEAD, width), LOW),
        jax.ShapeDtypeStruct((HEAD, width), LOW),
    ]
    return pl.pallas_call(
        project_kernel,
        grid_spec=pltpu.PrefetchScalarGridSpec(
            num_scalar_prefetch=1,
            grid=(rows // ROWS,),
            in_specs=[row_block(width), row_block(width), whole((8, 3 * HEAD))]
            + [table] * 3
            + [whole(slot.shape) for slot in slots],
            out_specs=[row_block(3 * HEAD), row_block(HEAD)]
            + [whole((3 * HEAD, width)), whole((HEAD, width))],
        ),
        out_shape=shapes,
        compiler_params=params(),
        cost_estimate=cost(8 * rows * width * HEAD, 4 * rows * width + 16 * HEAD * width),
        name="pr",
    )(chip, normed, grad_out, bias, *tables, *slots)


def head_grads_kernel(chip_ref, *refs):
    grad_joint_ref, attended_ref, normed_ref, grad_ref = refs[:4]
    slot_refs = refs[4:12]
    head_acc, dense_acc = refs[12:]
    chip = chip_ref[0]
    rows_of_head = head_acc.shape[0] // 8
    rows_of_dense = dense_acc.shape[0] // 8
    b = pl.program_id(0)

    @pl.when(b == 0)
    def _():
        head_acc[...] = jnp.zeros_like(head_acc)
        dense_acc[...] = jnp.zeros_like(dense_acc)

    head_acc[...] += dot_tn(grad_joint_ref[...], normed_ref[...])
    dense_acc[...] += dot_tn(attended_ref[...], grad_ref[...])

    @pl.when(b == pl.num_programs(0) - 1)
    def _():
        for ref, (bits, slabs) in zip(slot_refs, SINGLE_SLABS):
            for k, slab in enumerate(slabs):
                at = jnp.bitwise_xor(chip, bits) * 2 + slab
                head_at = pl.multiple_of(at * rows_of_head, 32)
                dense_at = pl.multiple_of(at * rows_of_dense, 32)
                ref[k, :rows_of_head, :] = head_acc[pl.ds(head_at, rows_of_head), :].astype(LOW)
                ref[k, rows_of_head:, :] = dense_acc[pl.ds(dense_at, rows_of_dense), :].astype(LOW)


def head_grads(chip, grad_joint, attended, normed, grad_out):
    rows, width = normed.shape
    slab = (1, HEAD // 2, width)
    return pl.pallas_call(
        head_grads_kernel,
        grid_spec=pltpu.PrefetchScalarGridSpec(
            num_scalar_prefetch=1,
            grid=(rows // ROWS,),
            in_specs=[row_block(3 * HEAD), row_block(HEAD), row_block(width), row_block(width)],
            out_specs=[whole(slab)] * 8,
            scratch_shapes=[pltpu.VMEM((3 * HEAD, width), F32), pltpu.VMEM((HEAD, width), F32)],
        ),
        out_shape=[jax.ShapeDtypeStruct(slab, LOW)] * 8,
        compiler_params=params(),
        cost_estimate=cost(8 * rows * width * HEAD, 4 * rows * width + 8 * HEAD * width),
        name="hg",
    )(chip, grad_joint, attended, normed, grad_out)


def attention_kernel(
    lens_ref,
    query_ref,
    grad_ref,
    cos_ref,
    after_ref,
    before_ref,
    attended_ref,
    grad_joint_ref,
    bias_ref,
    grad_key_s,
    grad_value_s,
):
    seq = pl.program_id(0)
    length = lens_ref[seq]
    length_all = query_ref.shape[0]
    tile = 256
    scale = HEAD ** (-0.5)
    grad_key_s[...] = jnp.zeros_like(grad_key_s)
    grad_value_s[...] = jnp.zeros_like(grad_value_s)

    @pl.when(seq == 0)
    def _():
        bias_ref[...] = jnp.zeros_like(bias_ref)

    for start in range(0, length_all, tile):
        rows = slice(start, start + tile)
        extent = start + tile

        @pl.when(start < length)
        def _(rows=rows, extent=extent, start=start):
            query = query_ref[rows, :HEAD]
            keys = query_ref[:extent, HEAD : 2 * HEAD]
            values = query_ref[:extent, 2 * HEAD :]
            grad = grad_ref[rows, :]
            scores = dot_nt(query, keys) * scale
            row_id = start + lax.broadcasted_iota(jnp.int32, scores.shape, 0)
            column_id = lax.broadcasted_iota(jnp.int32, scores.shape, 1)
            allowed = (column_id <= row_id) & (column_id < length)
            scores = jnp.where(allowed, scores, -1e30)
            weights = jnp.exp(scores - jnp.max(scores, axis=-1, keepdims=True))
            probs = weights / jnp.sum(weights, axis=-1, keepdims=True)
            probs_low = probs.astype(LOW)
            attended_ref[rows, :] = dot_nn(probs_low, values).astype(LOW)
            grad_probs = dot_nt(grad, values)
            delta = jnp.sum(probs * grad_probs, axis=-1, keepdims=True)
            grad_scores = (probs * (grad_probs - delta)).astype(LOW)
            tables = (cos_ref[rows, :], after_ref[rows, :], before_ref[rows, :])
            grad_query = turn_back(dot_nn(grad_scores, keys) * scale, *tables).astype(LOW)
            grad_joint_ref[rows, :HEAD] = grad_query
            grad_key_s[:extent, :] += dot_tn(grad_scores, query)
            grad_value_s[:extent, :] += dot_tn(probs_low, grad)
            bias_ref[0:1, :HEAD] += jnp.sum(grad_query.astype(F32), axis=0, keepdims=True)

        @pl.when(start >= length)
        def _(rows=rows):
            attended_ref[rows, :] = jnp.zeros((tile, HEAD), LOW)
            grad_joint_ref[rows, :HEAD] = jnp.zeros((tile, HEAD), LOW)

    for start in range(0, length_all, tile):
        rows = slice(start, start + tile)
        tables = (cos_ref[rows, :], after_ref[rows, :], before_ref[rows, :])
        grad_key = turn_back(grad_key_s[rows, :] * scale, *tables).astype(LOW)
        grad_value = grad_value_s[rows, :].astype(LOW)
        grad_joint_ref[rows, HEAD : 2 * HEAD] = grad_key
        grad_joint_ref[rows, 2 * HEAD :] = grad_value
        bias_ref[0:1, HEAD : 2 * HEAD] += jnp.sum(grad_key.astype(F32), axis=0, keepdims=True)
        bias_ref[0:1, 2 * HEAD :] += jnp.sum(grad_value.astype(F32), axis=0, keepdims=True)


def attention_both(lens, joint, grad_attended, tables, length_all):
    rows = joint.shape[0]
    seqs = rows // length_all

    def per_seq(width):
        return pl.BlockSpec((length_all, width), lambda s, *_: (s, 0))

    return pl.pallas_call(
        attention_kernel,
        grid_spec=pltpu.PrefetchScalarGridSpec(
            num_scalar_prefetch=1,
            grid=(seqs,),
            in_specs=[per_seq(3 * HEAD), per_seq(HEAD)] + [whole((length_all, 128))] * 3,
            out_specs=[per_seq(HEAD), per_seq(3 * HEAD), whole((8, 3 * HEAD))],
            scratch_shapes=[pltpu.VMEM((length_all, HEAD), F32)] * 2,
        ),
        out_shape=[
            jax.ShapeDtypeStruct((rows, HEAD), LOW),
            jax.ShapeDtypeStruct((rows, 3 * HEAD), LOW),
            jax.ShapeDtypeStruct((8, 3 * HEAD), F32),
        ],
        compiler_params=params(),
        cost_estimate=cost(12 * rows * length_all * HEAD, 14 * rows * HEAD, rows * length_all),
        name="attention_both",
    )(lens, joint, grad_attended, *tables)


def feed_kernel(length_all, pieces, lens_ref, *refs):
    mixed_ref, grad_ref, bias_ref = refs[:3]
    piece_refs = refs[3 : 3 + pieces]
    active_ref, grad_hidden_ref, bias_grad_ref = refs[3 + pieces : 6 + pieces]
    out_refs = refs[6 + pieces : 6 + 2 * pieces]
    up_s, down_s, up_acc, down_acc = refs[6 + 2 * pieces :]
    b = pl.program_id(0)

    @pl.when(b == 0)
    def _():
        at = 0
        for ref in piece_refs:
            for half in range(ref.shape[0]):
                up_s[at : at + 128, :] = ref[half, 0]
                down_s[at : at + 128, :] = ref[half, 1]
                at += 128
        up_acc[...] = jnp.zeros_like(up_acc)
        down_acc[...] = jnp.zeros_like(down_acc)
        bias_grad_ref[...] = jnp.zeros_like(bias_grad_ref)

    live = block_live(lens_ref, length_all)

    @pl.when(live)
    def _():
        mixed = mixed_ref[...]
        grad = grad_ref[...]
        hidden = dot_nt(mixed, up_s[...]) + bias_ref[0:1, :]
        gate = 0.5 * (1.0 + lax.erf(hidden * (2.0**-0.5)))
        active = (hidden * gate).astype(LOW)
        slope = gate + hidden * jnp.exp(-0.5 * hidden * hidden) * 0.3989422804014327
        grad_hidden32 = dot_nt(grad, down_s[...]) * slope
        grad_hidden = grad_hidden32.astype(LOW)
        active_ref[...] = active
        grad_hidden_ref[...] = grad_hidden
        bias_grad_ref[0:1, :] += jnp.sum(grad_hidden.astype(F32), axis=0, keepdims=True)
        down_acc[...] += dot_tn(active, grad)
        up_acc[...] += dot_tn(grad_hidden, mixed)

    @pl.when(jnp.logical_not(live))
    def _():
        active_ref[...] = jnp.zeros_like(active_ref)
        grad_hidden_ref[...] = jnp.zeros_like(grad_hidden_ref)

    @pl.when(b == pl.num_programs(0) - 1)
    def _():
        at = 0
        for ref in out_refs:
            for half in range(ref.shape[0]):
                ref[half, 0] = up_acc[at : at + 128, :].astype(LOW)
                ref[half, 1] = down_acc[at : at + 128, :].astype(LOW)
                at += 128


def feed_part(lens, mixed, grad_out, bias, pieces, length_all):
    rows, width = mixed.shape
    units = sum(128 * piece.shape[0] for piece in pieces)
    out = pl.pallas_call(
        partial(feed_kernel, length_all, len(pieces)),
        grid_spec=pltpu.PrefetchScalarGridSpec(
            num_scalar_prefetch=1,
            grid=(rows // ROWS,),
            in_specs=[row_block(width), row_block(width), whole((8, units))]
            + [whole(piece.shape) for piece in pieces],
            out_specs=[row_block(units), row_block(units), whole((8, units))]
            + [whole(piece.shape) for piece in pieces],
            scratch_shapes=[pltpu.VMEM((units, width), LOW)] * 2
            + [pltpu.VMEM((units, width), F32)] * 2,
        ),
        out_shape=[
            jax.ShapeDtypeStruct((rows, units), LOW),
            jax.ShapeDtypeStruct((rows, units), LOW),
            jax.ShapeDtypeStruct((8, units), F32),
        ]
        + [jax.ShapeDtypeStruct(piece.shape, LOW) for piece in pieces],
        compiler_params=params(),
        cost_estimate=cost(
            8 * rows * width * units, 4 * rows * width + 8 * units * width, 2 * rows * units
        ),
    )(lens, mixed, grad_out, jnp.broadcast_to(bias.astype(F32)[None, :], (8, units)), *pieces)
    return out[0], out[1], out[2][0], out[3:]


def output_kernel(seq, parts, pieces, lens_ref, *refs):
    active_refs = refs[: parts + 1]
    dense_ref = refs[parts + 1]
    piece_refs = refs[parts + 2 : parts + 2 + pieces]
    out_ref, down_s = refs[parts + 2 + pieces :]

    @pl.when(pl.program_id(0) == 0)
    def _():
        at = 0
        for ref in piece_refs:
            for half in range(ref.shape[0]):
                down_s[at : at + 128, :] = ref[half, 1]
                at += 128
        down_s[at : at + HEAD, :] = dense_ref[...]

    live = pl.program_id(0) * ROWS < lens_ref[seq]

    @pl.when(live)
    def _():
        left = jnp.concatenate([ref[...] for ref in active_refs], axis=1)
        out_ref[...] = dot_nn(left, down_s[...]).astype(LOW)

    @pl.when(jnp.logical_not(live))
    def _():
        out_ref[...] = jnp.zeros_like(out_ref)


def branch_output(lens, actives, attended, dense, pieces, length_all, seq):
    rows, width = length_all, dense.shape[1]
    units = sum(active.shape[1] for active in actives)
    return pl.pallas_call(
        partial(output_kernel, seq, len(actives), len(pieces)),
        grid_spec=pltpu.PrefetchScalarGridSpec(
            num_scalar_prefetch=1,
            grid=(rows // ROWS,),
            in_specs=[seq_block(active.shape[1], length_all, seq) for active in actives]
            + [seq_block(HEAD, length_all, seq), whole(dense.shape)]
            + [whole(piece.shape) for piece in pieces],
            out_specs=row_block(width),
            scratch_shapes=[pltpu.VMEM((units + HEAD, width), LOW)],
        ),
        out_shape=jax.ShapeDtypeStruct((rows, width), LOW),
        compiler_params=params(),
        cost_estimate=cost(
            2 * rows * width * (units + HEAD), 2 * rows * (width + units) + 4 * units * width
        ),
    )(lens, *actives, attended, dense, *pieces)


def swap(value, bit):
    size = lax.axis_size("dp")
    return lax.ppermute(value, "dp", [(k, k ^ bit) for k in range(size)])


def add_low(*terms):
    total = terms[0].astype(F32)
    for term in terms[1:]:
        total = total + term.astype(F32)
    return total


def chain_steps(parts, one_ref, two_ref, out_ref, sent_s, got_s, send_sems, recv_sems):
    size = lax.axis_size("tensor")
    here = lax.axis_index("tensor")
    rows, width = out_ref.shape[0] // parts, out_ref.shape[1]
    total = (size - 1) * parts
    below, above = here > 0, here < size - 1
    up, down = lax.min(here + 1, size - 1), lax.max(here - 1, 0)
    mesh_id = pl.DeviceIdType.MESH

    def copy(way, item):
        return pltpu.make_async_remote_copy(
            src_ref=sent_s.at[way, item],
            dst_ref=got_s.at[way, item],
            send_sem=send_sems.at[way, item],
            recv_sem=recv_sems.at[way, item],
            device_id={"tensor": down if way else up},
            device_id_type=mesh_id,
        )

    def own(shard, part):
        at = (
            pl.ds(pl.multiple_of(part * rows, rows), rows),
            pl.ds(pl.multiple_of(shard * width, width), width),
        )
        return one_ref[at].astype(F32) + two_ref[at].astype(F32)

    def shard_of(way, item):
        turn = item // parts
        return turn if way else size - 1 - turn

    def sends(way, item):
        shard = shard_of(way, item)
        return (item >= 0) & (item < total) & ((shard < here) if way else (shard > here))

    def greet():
        barrier = pltpu.get_barrier_semaphore()

        @pl.when(below)
        def _():
            pl.semaphore_signal(barrier, inc=1, device_id={"tensor": down}, device_id_type=mesh_id)

        @pl.when(above)
        def _():
            pl.semaphore_signal(barrier, inc=1, device_id={"tensor": up}, device_id_type=mesh_id)

        pl.semaphore_wait(barrier, lax.select(below & above, jnp.int32(2), jnp.int32(1)))

    def step(time, unused):
        for way in range(2):
            first = above if way else below
            item = time - (size - 1 - here if way else here)

            @pl.when(sends(way, item))
            def _(way=way, item=item, first=first):
                part = item % parts
                value = own(shard_of(way, item), part)

                @pl.when(first)
                def _():
                    copy(way, item).wait_recv()
                    sent_s[way, item] = (value + got_s[way, item].astype(F32)).astype(LOW)

                @pl.when(jnp.logical_not(first))
                def _():
                    sent_s[way, item] = value.astype(LOW)

                copy(way, item).start()

        return unused

    def finish(part, unused):
        at = pl.ds(pl.multiple_of(part * rows, rows), rows)
        out_ref[at, :] = own(here, part)
        for way in range(2):
            turn = here if way else size - 1 - here

            @pl.when(above if way else below)
            def _(way=way, turn=turn):
                item = turn * parts + part
                copy(way, item).wait_recv()
                out_ref[at, :] += got_s[way, item].astype(F32)

        return unused

    def drain(item, unused):
        for way in range(2):

            @pl.when(sends(way, item))
            def _(way=way):
                copy(way, item).wait_send()

        return unused

    def close(start):
        lax.fori_loop(start, total + size - 1, step, 0)
        lax.fori_loop(0, parts, finish, 0)
        lax.fori_loop(0, total, drain, 0)

    return greet, step, close


def chain_kernel(parts, *refs):
    greet, _, close = chain_steps(parts, *refs)
    greet()
    close(0)


def chain_scratch(rows, width):
    size = lax.axis_size("tensor")
    slots = (2, (size - 1) * PARTS, rows // PARTS, width // size)
    return [
        pltpu.VMEM(slots, LOW),
        pltpu.VMEM(slots, LOW),
        pltpu.SemaphoreType.DMA(slots[:2]),
        pltpu.SemaphoreType.DMA(slots[:2]),
    ]


def input_grads_kernel(parts, pieces, *refs):
    grad_refs = refs[:parts]
    grad_joint_ref, own_ref, other_ref, affine_ref, qkv_ref = refs[parts : parts + 5]
    piece_refs = refs[parts + 5 : parts + 5 + pieces]
    rest = refs[parts + 5 + pieces :]
    branch_refs, (out_own_ref, out_other_ref, norm_ref, total_ref) = rest[:2], rest[2:6]
    up_s, one_s, two_s = rest[6:9]
    greet, step, close = chain_steps(PARTS, *branch_refs, total_ref, *rest[9:])
    b = pl.program_id(0)
    steps = pl.num_programs(0)

    @pl.when(b == 0)
    def _():
        greet()

    step(b, 0)

    @pl.when(b == 0)
    def _():
        for k, ref in enumerate(piece_refs):
            up_s[128 * k : 128 * k + 128, :] = ref[0, 0]
        norm_ref[...] = jnp.zeros_like(norm_ref)

    one_s[...] = dot_nn(grad_joint_ref[...], qkv_ref[...])
    left = jnp.concatenate([ref[...] for ref in grad_refs], axis=1)
    two_s[...] = dot_nn(left, up_s[...])
    is_other = b < steps // 2
    unit, inverse = unit_rows(jnp.where(is_other, other_ref[...], own_ref[...]))
    grad_one, grad_two = one_s[...], two_s[...]
    first, second = grad_one * unit, grad_two * unit
    norm_ref[0:1, :] += jnp.sum(first, axis=0, keepdims=True)
    norm_ref[1:2, :] += jnp.sum(grad_one, axis=0, keepdims=True)
    norm_ref[2:3, :] += jnp.sum(second, axis=0, keepdims=True)
    norm_ref[3:4, :] += jnp.sum(grad_two, axis=0, keepdims=True)
    gain_one, gain_two = affine_ref[0:1, :], affine_ref[2:3, :]
    scaled = grad_one * gain_one + grad_two * gain_two
    along = jnp.mean(first * gain_one + second * gain_two, axis=-1, keepdims=True)
    scaled_mean = jnp.mean(scaled, axis=-1, keepdims=True)
    result = (inverse * (scaled - scaled_mean - unit * along)).astype(LOW)

    @pl.when(is_other)
    def _():
        out_other_ref[...] = result

    @pl.when(jnp.logical_not(is_other))
    def _():
        out_own_ref[...] = result

    @pl.when(b == steps - 1)
    def _():
        close(steps)


def input_grads_and_chain(grads, grad_joint, own, other, affine, qkv, pieces, branches):
    rows, width = own.shape
    size = lax.axis_size("tensor")
    block = 256
    half = rows // block
    units = sum(grad.shape[1] for grad in grads)

    def turned(columns):
        return pl.BlockSpec((block, columns), lambda b: ((b + half) % (2 * half), 0))

    def own_block():
        return pl.BlockSpec((block, width), lambda b: (jnp.maximum(b - half, 0), 0))

    def other_block():
        return pl.BlockSpec((block, width), lambda b: (jnp.minimum(b, half - 1), 0))

    piece_spec = pl.BlockSpec(
        (1, 1, 128, width), lambda b: (0, 0, 0, 0), pipeline_mode=pl.Buffered(1)
    )
    return pl.pallas_call(
        partial(input_grads_kernel, len(grads), len(pieces)),
        grid=(2 * half,),
        in_specs=[turned(grad.shape[1]) for grad in grads]
        + [turned(3 * HEAD), own_block(), other_block(), whole((8, width)), whole(qkv.shape)]
        + [piece_spec] * len(pieces)
        + [whole((rows, width))] * 2,
        out_specs=[own_block(), other_block(), whole((8, width)), whole((rows, width // size))],
        out_shape=[
            jax.ShapeDtypeStruct((rows, width), LOW),
            jax.ShapeDtypeStruct((rows, width), LOW),
            jax.ShapeDtypeStruct((8, width), F32),
            jax.ShapeDtypeStruct((rows, width // size), F32),
        ],
        scratch_shapes=[pltpu.VMEM((units, width), LOW)]
        + [pltpu.VMEM((block, width), F32)] * 2
        + chain_scratch(rows, width),
        compiler_params=pltpu.CompilerParams(
            dimension_semantics=("arbitrary",),
            collective_id=1,
            has_side_effects=True,
            vmem_limit_bytes=64 * 1024 * 1024 - 65536,
        ),
        cost_estimate=cost(4 * rows * width * (units + 3 * HEAD), 16 * rows * width),
    )(*grads, grad_joint, own, other, affine, qkv, *pieces, *branches)


def chain_in_kernel(one, two):
    size = lax.axis_size("tensor")
    rows, width = one.shape
    return pl.pallas_call(
        partial(chain_kernel, PARTS),
        in_specs=[pl.BlockSpec(memory_space=pltpu.VMEM)] * 2,
        out_specs=pl.BlockSpec(memory_space=pltpu.VMEM),
        out_shape=jax.ShapeDtypeStruct((rows, width // size), F32),
        scratch_shapes=chain_scratch(rows, width),
        compiler_params=pltpu.CompilerParams(
            collective_id=0, has_side_effects=True, vmem_limit_bytes=VMEM_LIMIT
        ),
        cost_estimate=cost(2 * rows * width, 8 * rows * width),
    )(one, two)


def small_scatter(value, axis, bits):
    place = lax.axis_index(axis)
    size = lax.axis_size(axis)
    for bit in bits:
        half = value.shape[0] // 2
        upper = (place // bit) % 2
        mine = lax.dynamic_slice_in_dim(value, upper * half, half, 0)
        theirs = lax.dynamic_slice_in_dim(value, (1 - upper) * half, half, 0)
        value = mine + lax.ppermute(theirs, axis, [(k, k ^ bit) for k in range(size)])
    return value[0]


def local_fast(
    tokens,
    cotangent,
    lengths,
    keep,
    first_gain,
    first_shift,
    second_gain,
    second_shift,
    qkv_weight,
    qkv_bias,
    dense_weight,
    up_weight,
    up_bias,
    down_weight,
    branch_bias,
):
    tokens, cotangent, keep = tokens[0], cotangent[0], keep[0]
    length_all, width = tokens.shape
    place = lax.axis_index("dp")
    core, chip = place % 2, place // 2
    dp_size, tensor_size = lax.axis_size("dp"), lax.axis_size("tensor")
    qkv_rows, units = qkv_weight.shape[1], up_weight.shape[0]
    positions = jnp.arange(length_all)
    live = positions < lengths[0]
    valid = (live & (keep == 1)).astype(F32)
    chips = chip.astype(jnp.int32)[None]

    def head_rows(head):
        return jnp.concatenate(
            [
                lax.dynamic_index_in_dim(qkv_weight, head, 0, False),
                lax.dynamic_index_in_dim(dense_weight, head, 0, False),
            ],
            axis=0,
        )

    def by_core(mine, other):
        pair = jnp.zeros((2,) + mine.shape, mine.dtype)
        pair = lax.dynamic_update_index_in_dim(pair, mine, core, 0)
        return lax.dynamic_update_index_in_dim(pair, other, 1 - core, 0)

    head_own = by_core(head_rows(core), swap(head_rows(1 - core), 1))
    head_x, head_y = swap(head_own, 2), swap(head_own, 4)
    head_d0, head_d1 = swap(head_y[:1], 2), swap(head_x[1:], 4)
    slots = (head_own, head_x, head_y, head_d0, head_d1)

    other_tokens = swap(tokens, 1)
    other_cotangent = swap(cotangent, 1)
    facts = jnp.concatenate([valid, jnp.full((128,), 1.0, F32) * lengths[0].astype(F32)])[None]
    other_facts = swap(facts, 1)
    lens = jnp.stack([lengths[0], other_facts[0, length_all].astype(jnp.int32)])
    affine = jnp.stack([first_gain, first_shift, second_gain, second_shift] * 2)
    firsts = both_norms(tokens, cotangent, valid[:, None], affine, (), 0)
    up_weight, down_weight, positions, _ = lax.optimization_barrier(
        (up_weight, down_weight, positions, firsts[0])
    )
    biases = jnp.concatenate([up_bias, qkv_bias.reshape(-1)])
    biases = jnp.pad(biases, (0, -biases.shape[0] % 128))[None]
    for bit in (1, 2, 4):
        biases = jnp.concatenate([biases, swap(biases, bit)], axis=0)
    up_biases = biases[:, :units]
    qkv_biases = biases[:, units : units + 2 * qkv_rows].reshape(dp_size, 2, qkv_rows)
    qkv_biases = lax.dynamic_index_in_dim(qkv_biases, core, 1, False)
    qkv_bias_head = qkv_biases[place ^ jnp.arange(dp_size)].reshape(-1).astype(F32)
    qkv_bias_head = jnp.broadcast_to(qkv_bias_head[None], (8, 3 * HEAD))

    normed, mixed, grad_out = both_norms(
        other_tokens, other_cotangent, other_facts[0, :length_all][:, None], affine, firsts, 1
    )

    up_halves = up_weight.reshape(2, 1, units // 2, width)
    down_halves = down_weight.reshape(2, 1, units // 2, width)
    feed_0 = jnp.stack([up_halves[0], down_halves[0]], axis=1)
    feed_1 = jnp.stack([up_halves[1], down_halves[1]], axis=1)
    feed_x0, feed_y0 = swap(feed_0, 2), swap(feed_0, 4)
    feed_x1, feed_y1 = swap(feed_1, 2), swap(feed_1, 4)
    feed_d0, feed_d1 = swap(feed_y0, 2), swap(feed_x1, 4)

    def feed(pieces, bias):
        bias = jnp.concatenate(bias)
        return feed_part(lens, mixed, grad_out, bias, pieces, length_all)

    low_units, high_units = slice(0, units // 2), slice(units // 2, units)
    feed_a = feed([feed_0, feed_1], [up_biases[0]])

    cosine, sine = rotary_tables(positions[0].astype(F32), length_all)
    cosine, sine = cosine[:, 0], sine[:, 0]
    half = ROT // 2
    zeros = jnp.zeros((length_all, 128 - ROT), F32)
    blank = jnp.zeros((length_all, half), F32)
    tables = (
        jnp.concatenate([cosine, zeros + 1.0], axis=1),
        jnp.concatenate([blank, sine[:, half:], zeros], axis=1),
        jnp.concatenate([-sine[:, :half], blank, zeros], axis=1),
    )
    query_key_value, grad_attended, qkv_full, dense_full = project(
        chips, normed, grad_out, qkv_bias_head, tables, slots, length_all
    )
    attended, grad_joint, bias_joint = attention_both(
        lens, query_key_value, grad_attended, tables, length_all
    )
    slot_grads = head_grads(chips, grad_joint, attended, normed, grad_out)

    feed_b = feed(
        [feed_x0, feed_y0, feed_x1, feed_y1, feed_d0, feed_d1],
        [up_biases[2, low_units], up_biases[4, low_units]]
        + [up_biases[2, high_units], up_biases[4, high_units], up_biases[6]],
    )
    feeds = (feed_a, feed_b)
    pieces = [feed_0, feed_1, feed_x0, feed_y0, feed_x1, feed_y1, feed_d0, feed_d1]

    def branch_of(seq):
        actives = [item[0] for item in feeds]
        return branch_output(lens, actives, attended, dense_full, pieces, length_all, seq)

    branch_other = swap(branch_of(1), 1)
    branch_own = branch_of(0)

    grad_x_own, grad_x_other, norm_sums, branch_total = input_grads_and_chain(
        [item[1] for item in feeds],
        grad_joint,
        tokens,
        other_tokens,
        affine,
        qkv_full,
        pieces,
        (branch_own, branch_other),
    )
    grad_x_other = swap(grad_x_other, 1)
    slice_width = width // tensor_size
    column_start = lax.axis_index("tensor") * slice_width
    token_slice = lax.dynamic_slice_in_dim(tokens, column_start, slice_width, 1).astype(F32)
    bias_slice = lax.dynamic_slice_in_dim(branch_bias, column_start, slice_width, 0)
    block_out = (token_slice + jnp.where(live[:, None], branch_total + bias_slice, 0.0)).astype(LOW)

    grad_x_total = chain_in_kernel(grad_x_own, grad_x_other)
    grad_slice = lax.dynamic_slice_in_dim(cotangent, column_start, slice_width, 1).astype(F32)
    input_grad = (grad_slice * valid[:, None] + grad_x_total).astype(LOW)

    def scatter(own, over_x, over_y, far):
        through_x = swap(far[0], 2)
        through_y = swap(far[1], 4)
        over_y = (add_low(over_y[0], through_x).astype(LOW), over_y[1])
        over_x = (over_x[0], add_low(over_x[1], through_y).astype(LOW))
        from_x = [swap(item, 2) for item in over_x]
        from_y = [swap(item, 4) for item in over_y]
        return [add_low(own[k], from_x[k], from_y[k]) for k in range(2)]

    grad_a, (over_x0, over_y0, over_x1, over_y1, *far) = feed_a[3], feed_b[3]
    feed_grad = scatter(grad_a, (over_x0, over_x1), (over_y0, over_y1), far)
    up_grad_out = jnp.concatenate([item[0, 0] for item in feed_grad], axis=0)
    down_grad_out = jnp.concatenate([item[0, 1] for item in feed_grad], axis=0)

    head_grad = jnp.concatenate(scatter(*[slot_grads[2 * k : 2 * k + 2] for k in range(4)]), axis=0)
    head_mine = lax.dynamic_index_in_dim(head_grad, core, 0, False)
    head_other = lax.dynamic_index_in_dim(head_grad, 1 - core, 0, False)
    head_other = swap(head_other.astype(LOW), 1).astype(F32)
    head_out = by_core(head_mine, head_other)
    qkv_grad_out, dense_grad_out = head_out[:, :qkv_rows], head_out[:, qkv_rows:]

    (bias_own, bias_rest, bias_joint, grad_rows), norm_sums = lax.optimization_barrier(
        ((feed_a[2], feed_b[2], bias_joint, grad_out), norm_sums)
    )
    rest = bias_rest.reshape(6, units // 2)
    column_bias = jnp.stack(
        [
            bias_own,
            jnp.concatenate([rest[0], rest[2]]),
            jnp.concatenate([rest[1], rest[3]]),
            jnp.concatenate([rest[4], rest[5]]),
        ]
    )[chip ^ jnp.arange(4)]
    column_bias = jnp.stack(
        [jnp.where(core == 0, column_bias, 0.0), jnp.where(core == 0, 0.0, column_bias)], axis=1
    ).reshape(dp_size, units)
    head_bias = bias_joint[0].reshape(dp_size, qkv_rows)
    head_bias = jnp.concatenate(
        [jnp.where(core == 0, head_bias, 0.0), jnp.where(core == 0, 0.0, head_bias)], axis=1
    )
    row_width = length_all // tensor_size
    bias_term = jnp.sum(
        lax.dynamic_slice_in_dim(
            grad_rows, lax.axis_index("tensor") * row_width, row_width, 0
        ).astype(F32),
        axis=0,
    )
    norm_rows = jnp.concatenate([norm_sums[:4], bias_term[None]], axis=0)
    norm_rows = norm_rows.reshape(5, dp_size, -1).transpose(1, 0, 2).reshape(dp_size, -1)
    small = jnp.concatenate([column_bias, head_bias, norm_rows], axis=1)
    small = jnp.pad(small, ((0, 0), (0, -small.shape[1] % 128)))
    small = small_scatter(small, "dp", (4, 2, 1))
    up_bias_grad_out = small[:units]
    qkv_bias_grad_out = small[units : units + 2 * qkv_rows].reshape(2, qkv_rows)
    at = units + 2 * qkv_rows
    norms = small[at : at + 5 * width // dp_size].reshape(5, tensor_size, -1).transpose(1, 0, 2)
    bits = [1 << k for k in reversed(range(tensor_size.bit_length() - 1))]
    norms_out = small_scatter(norms.reshape(tensor_size, -1), "tensor", bits).reshape(5, -1)
    return (
        block_out[None],
        input_grad[None],
        qkv_grad_out,
        qkv_bias_grad_out,
        dense_grad_out,
        up_grad_out,
        up_bias_grad_out,
        down_grad_out,
        norms_out,
    )


def solution(mesh):
    in_specs = (
        P("dp", None, None),
        P("dp", None, None),
        P("dp"),
        P("dp", None),
        P(),
        P(),
        P(),
        P(),
        P("tensor", "dp", None),
        P("tensor", "dp"),
        P("tensor", "dp", None),
        P(("dp", "tensor"), None),
        P(("dp", "tensor")),
        P(("dp", "tensor"), None),
        P(),
    )
    out_specs = (
        P("dp", None, "tensor"),
        P("dp", None, "tensor"),
        P("tensor", "dp", None),
        P("tensor", "dp"),
        P("tensor", "dp", None),
        P(("dp", "tensor"), None),
        P(("dp", "tensor")),
        P(("dp", "tensor"), None),
        P(None, ("dp", "tensor")),
    )

    fits = mesh.shape["dp"] == 8 and mesh.shape["tensor"] * 2 == HEADS

    def local(*items):
        return (local_fast if fits else local_general)(*items)

    return jax.shard_map(local, mesh=mesh, in_specs=in_specs, out_specs=out_specs, check_vma=False)
```

```python
from functools import partial

import jax
import jax.numpy as jnp
from jax import lax
from jax.experimental import pallas as pl
from jax.experimental.pallas import tpu as pltpu
from jax.sharding import PartitionSpec as P


HEADS = 8
HEAD = 256
ROT = 64
BLOCK = 512


def layer_norm_parts(values, gain, shift):
    centred = values - jnp.mean(values, axis=-1, keepdims=True)
    inverse = lax.rsqrt(jnp.mean(centred * centred, axis=-1, keepdims=True) + 1e-05)
    unit = centred * inverse
    return (unit * gain + shift, unit, inverse)


def norm_back(grad, unit, inverse, gain):
    scaled = grad * gain
    centred = scaled - jnp.mean(scaled, axis=-1, keepdims=True)
    return inverse * (centred - unit * jnp.mean(scaled * unit, axis=-1, keepdims=True))


def rotary_tables(start, count):
    half = ROT // 2
    inverse = 10000.0 ** (-jnp.arange(half, dtype=jnp.float32) * 2.0 / ROT)
    angles = (start + jnp.arange(count, dtype=jnp.float32))[:, None] * inverse[None, :]
    angles = jnp.concatenate([angles, angles], axis=1)
    return (jnp.cos(angles)[:, None, :], jnp.sin(angles)[:, None, :])


def rotate(values, cosine, sine):
    half = ROT // 2
    part = values[..., :ROT]
    turned = jnp.concatenate([-part[..., half:], part[..., :half]], axis=-1)
    return jnp.concatenate([part * cosine + turned * sine, values[..., ROT:]], axis=-1)


def rotate_back(grad, cosine, sine):
    half = ROT // 2
    part = grad[..., :ROT]
    scaled = part * sine
    turned = jnp.concatenate([scaled[..., half:], -scaled[..., :half]], axis=-1)
    return jnp.concatenate([part * cosine + turned, grad[..., ROT:]], axis=-1)


def block_scores(query_block, key_rows, query_start, key_start, length):
    scores = jnp.einsum(
        "qhe,khe->hqk", query_block, key_rows, preferred_element_type=jnp.float32
    ) * HEAD ** (-0.5)
    rows = query_start + jnp.arange(query_block.shape[0])
    columns = key_start + jnp.arange(key_rows.shape[0])
    allowed = (columns[None, :] <= rows[:, None]) & (columns[None, :] < length)
    return jnp.where(allowed[None], scores, -1e30)


def when_live(flag, work, operand):
    return lax.cond(flag, work, lambda unused: jax.tree.map(jnp.zeros_like, work(unused)), operand)


def local_general(
    tokens,
    cotangent,
    lengths,
    keep,
    first_gain,
    first_shift,
    second_gain,
    second_shift,
    qkv_weight,
    qkv_bias,
    dense_weight,
    up_weight,
    up_bias,
    down_weight,
    branch_bias,
):
    gathered = (
        lax.all_gather(qkv_weight, "dp", axis=1, tiled=True),
        lax.all_gather(qkv_bias, "dp", axis=1, tiled=True),
        lax.all_gather(dense_weight, "dp", axis=1, tiled=True),
        lax.all_gather(up_weight, "dp", axis=0, tiled=True),
        lax.all_gather(up_bias, "dp", axis=0, tiled=True),
        lax.all_gather(down_weight, "dp", axis=0, tiled=True),
    )
    qkv_full, qkv_bias_full, dense_full, up_full, up_bias_full, down_full = gathered
    _, length_all, width = tokens.shape
    blocks = length_all // BLOCK
    heads_here = qkv_full.shape[0]
    hidden_here = up_full.shape[0]
    scale = HEAD ** (-0.5)
    positions = jnp.arange(length_all)
    live_rows = positions[None, :] < lengths[:, None]

    def forward_one(items):
        row_tokens, length = items
        dense_flat = dense_full.reshape(heads_here * HEAD, width)

        def project(row_block, start):
            values32 = row_block.astype(jnp.float32)
            normed = layer_norm_parts(values32, first_gain, first_shift)[0].astype(jnp.bfloat16)
            joint = jnp.einsum(
                "bd,hed->bhe", normed, qkv_full, preferred_element_type=jnp.float32
            ) + qkv_bias_full.astype(jnp.float32)
            cosine, sine = rotary_tables(start, BLOCK)
            query_rows = rotate(joint[..., :HEAD], cosine, sine).astype(jnp.bfloat16)
            key_rows = rotate(joint[..., HEAD : 2 * HEAD], cosine, sine).astype(jnp.bfloat16)
            value_rows = joint[..., 2 * HEAD :].astype(jnp.bfloat16)
            mixed = layer_norm_parts(values32, second_gain, second_shift)[0].astype(jnp.bfloat16)
            hidden_rows = jnp.einsum(
                "bd,fd->bf", mixed, up_full, preferred_element_type=jnp.float32
            ) + up_bias_full.astype(jnp.float32)
            active = jax.nn.gelu(hidden_rows, approximate=False).astype(jnp.bfloat16)
            feed = jnp.dot(active, down_full, preferred_element_type=jnp.float32)
            return (query_rows, key_rows, value_rows, hidden_rows, feed)

        outputs = []
        for index in range(blocks):
            start = index * BLOCK
            outputs.append(
                when_live(
                    start < length, partial(project, start=start), row_tokens[start : start + BLOCK]
                )
            )
        query_all = jnp.concatenate([item[0] for item in outputs], axis=0)
        keys_all = jnp.concatenate([item[1] for item in outputs], axis=0)
        values_all = jnp.concatenate([item[2] for item in outputs], axis=0)
        hidden_all = jnp.concatenate([item[3] for item in outputs], axis=0)
        feed_all = jnp.concatenate([item[4] for item in outputs], axis=0)

        def attend(query_block, start):
            peak = jnp.full((heads_here, BLOCK, 1), -1e30, jnp.float32)
            total = jnp.zeros((heads_here, BLOCK, 1), jnp.float32)
            for key_index in range(start // BLOCK + 1):
                key_start = key_index * BLOCK
                scores = block_scores(
                    query_block, keys_all[key_start : key_start + BLOCK], start, key_start, length
                )
                newer = jnp.maximum(peak, jnp.max(scores, axis=-1, keepdims=True))
                total = total * jnp.exp(peak - newer) + jnp.sum(
                    jnp.exp(scores - newer), axis=-1, keepdims=True
                )
                peak = newer
            logsum = peak + jnp.log(total)
            summed = jnp.zeros((BLOCK, heads_here, HEAD), jnp.float32)
            for key_index in range(start // BLOCK + 1):
                key_start = key_index * BLOCK
                scores = block_scores(
                    query_block, keys_all[key_start : key_start + BLOCK], start, key_start, length
                )
                probs = jnp.exp(scores - logsum).astype(jnp.bfloat16)
                summed = summed + jnp.einsum(
                    "hqk,khe->qhe",
                    probs,
                    values_all[key_start : key_start + BLOCK],
                    preferred_element_type=jnp.float32,
                )
            attended_block = summed.astype(jnp.bfloat16).reshape(BLOCK, heads_here * HEAD)
            attention_rows = jnp.dot(attended_block, dense_flat, preferred_element_type=jnp.float32)
            return (attended_block, logsum[..., 0], attention_rows)

        pieces = []
        for index in range(blocks):
            start = index * BLOCK
            pieces.append(
                when_live(
                    start < length, partial(attend, start=start), query_all[start : start + BLOCK]
                )
            )
        attended_all = jnp.concatenate([item[0] for item in pieces], axis=0)
        logsum_all = jnp.concatenate([item[1] for item in pieces], axis=1)
        attention_all = jnp.concatenate([item[2] for item in pieces], axis=0)
        live = (positions < length)[:, None]
        branch_part = jnp.where(live, attention_all + feed_all, 0.0)
        return (branch_part, query_all, keys_all, values_all, hidden_all, attended_all, logsum_all)

    branch_part, query_all, keys_all, values_all, hidden_all, attended_all, logsum_all = lax.map(
        forward_one, (tokens, lengths)
    )
    branch_total = lax.psum_scatter(branch_part, "tensor", scatter_dimension=2, tiled=True)
    slice_width = branch_total.shape[2]
    column_start = lax.axis_index("tensor") * slice_width
    token_slice = lax.dynamic_slice_in_dim(tokens, column_start, slice_width, 2).astype(jnp.float32)
    bias_slice = lax.dynamic_slice_in_dim(branch_bias, column_start, slice_width, 0)
    block_out = (
        token_slice + jnp.where(live_rows[..., None], branch_total + bias_slice, 0.0)
    ).astype(jnp.bfloat16)
    qkv_back, dense_back, up_back, down_back = (
        lax.all_gather(qkv_weight, "dp", axis=1, tiled=True),
        lax.all_gather(dense_weight, "dp", axis=1, tiled=True),
        lax.all_gather(up_weight, "dp", axis=0, tiled=True),
        lax.all_gather(down_weight, "dp", axis=0, tiled=True),
    )
    dense_back_flat = dense_back.reshape(heads_here * HEAD, width)
    valid = live_rows & (keep == 1)
    grad_out = jnp.where(valid[..., None], cotangent, jnp.zeros((), jnp.bfloat16))
    row_width = length_all // lax.axis_size("tensor")
    row_start = lax.axis_index("tensor") * row_width
    bias_term = jnp.sum(
        lax.dynamic_slice_in_dim(grad_out, row_start, row_width, 1).astype(jnp.float32), axis=(0, 1)
    )

    def feed_back(carry, items):
        row_tokens, row_grad, row_hidden, length = items
        outputs = []
        for index in range(blocks):
            start = index * BLOCK

            def work(operand, start=start):
                grad_up, grad_up_bias, grad_down, gain_two, shift_two = operand
                values32 = row_tokens[start : start + BLOCK].astype(jnp.float32)
                normed, unit, inverse = layer_norm_parts(values32, second_gain, second_shift)
                mixed = normed.astype(jnp.bfloat16)
                grad_rows = row_grad[start : start + BLOCK]
                hidden_rows = row_hidden[start : start + BLOCK]
                grad_active = jnp.einsum(
                    "bd,fd->bf", grad_rows, down_back, preferred_element_type=jnp.float32
                )
                active, gelu_back = jax.vjp(partial(jax.nn.gelu, approximate=False), hidden_rows)
                grad_hidden = gelu_back(grad_active)[0].astype(jnp.bfloat16)
                grad_down = grad_down + jnp.einsum(
                    "bf,bd->fd",
                    active.astype(jnp.bfloat16),
                    grad_rows,
                    preferred_element_type=jnp.float32,
                )
                grad_up = grad_up + jnp.einsum(
                    "bf,bd->fd", grad_hidden, mixed, preferred_element_type=jnp.float32
                )
                grad_up_bias = grad_up_bias + jnp.sum(grad_hidden.astype(jnp.float32), axis=0)
                grad_mixed = jnp.dot(grad_hidden, up_back, preferred_element_type=jnp.float32)
                gain_two = gain_two + jnp.sum(grad_mixed * unit, axis=0)
                shift_two = shift_two + jnp.sum(grad_mixed, axis=0)
                return (
                    (grad_up, grad_up_bias, grad_down, gain_two, shift_two),
                    norm_back(grad_mixed, unit, inverse, second_gain),
                )

            carry, piece = lax.cond(
                start < length,
                work,
                lambda operand: (operand, jnp.zeros((BLOCK, width), jnp.float32)),
                carry,
            )
            outputs.append(piece)
        return (carry, jnp.concatenate(outputs, axis=0))

    feed_init = (
        jnp.zeros((hidden_here, width), jnp.float32),
        jnp.zeros((hidden_here,), jnp.float32),
        jnp.zeros((hidden_here, width), jnp.float32),
        jnp.zeros((width,), jnp.float32),
        jnp.zeros((width,), jnp.float32),
    )
    feed_totals, grad_x_two = lax.scan(
        feed_back, feed_init, (tokens, grad_out, hidden_all, lengths)
    )
    grad_up_total, grad_up_bias_total, grad_down_total, gain_two, shift_two = feed_totals

    def attention_back(carry, items):
        (
            row_tokens,
            row_grad,
            query_rows,
            key_rows,
            value_rows,
            attended_rows,
            logsum_rows,
            length,
        ) = items
        grad_qkv, grad_qkv_bias, grad_dense, gain_one, shift_one = carry
        grad_attended = jnp.einsum(
            "ld,nd->ln", row_grad, dense_back_flat, preferred_element_type=jnp.float32
        ).astype(jnp.bfloat16)
        grad_dense = grad_dense + jnp.einsum(
            "ln,ld->nd", attended_rows, row_grad, preferred_element_type=jnp.float32
        )
        grad_attended = grad_attended.reshape(length_all, heads_here, HEAD)
        grad_keys = jnp.zeros((length_all, heads_here, HEAD), jnp.float32)
        grad_values = jnp.zeros((length_all, heads_here, HEAD), jnp.float32)
        query_grads = []
        for query_index in range(blocks):
            query_start = query_index * BLOCK

            def work(operand, query_start=query_start, query_index=query_index):
                grad_keys_now, grad_values_now = operand
                query_block = query_rows[query_start : query_start + BLOCK]
                grad_block = grad_attended[query_start : query_start + BLOCK]
                logsum_block = logsum_rows[:, query_start : query_start + BLOCK][..., None]

                def probs_and_grad(key_start):
                    scores = block_scores(
                        query_block,
                        key_rows[key_start : key_start + BLOCK],
                        query_start,
                        key_start,
                        length,
                    )
                    probs = jnp.exp(scores - logsum_block)
                    grad_probs = jnp.einsum(
                        "qhe,khe->hqk",
                        grad_block,
                        value_rows[key_start : key_start + BLOCK],
                        preferred_element_type=jnp.float32,
                    )
                    return (probs, grad_probs)

                delta = jnp.zeros((heads_here, BLOCK, 1), jnp.float32)
                for key_index in range(query_index + 1):
                    probs, grad_probs = probs_and_grad(key_index * BLOCK)
                    delta = delta + jnp.sum(probs * grad_probs, axis=-1, keepdims=True)
                grad_query_block = jnp.zeros((BLOCK, heads_here, HEAD), jnp.float32)
                for key_index in range(query_index + 1):
                    key_start = key_index * BLOCK
                    probs, grad_probs = probs_and_grad(key_start)
                    grad_scores = (probs * (grad_probs - delta)).astype(jnp.bfloat16)
                    grad_query_block = (
                        grad_query_block
                        + jnp.einsum(
                            "hqk,khe->qhe",
                            grad_scores,
                            key_rows[key_start : key_start + BLOCK],
                            preferred_element_type=jnp.float32,
                        )
                        * scale
                    )
                    grad_keys_now = grad_keys_now.at[key_start : key_start + BLOCK].add(
                        jnp.einsum(
                            "hqk,qhe->khe",
                            grad_scores,
                            query_block,
                            preferred_element_type=jnp.float32,
                        )
                        * scale
                    )
                    grad_values_now = grad_values_now.at[key_start : key_start + BLOCK].add(
                        jnp.einsum(
                            "hqk,qhe->khe",
                            probs.astype(jnp.bfloat16),
                            grad_block,
                            preferred_element_type=jnp.float32,
                        )
                    )
                return ((grad_keys_now, grad_values_now), grad_query_block)

            (grad_keys, grad_values), query_piece = lax.cond(
                query_start < length,
                work,
                lambda operand: (operand, jnp.zeros((BLOCK, heads_here, HEAD), jnp.float32)),
                (grad_keys, grad_values),
            )
            query_grads.append(query_piece)
        grad_query = jnp.concatenate(query_grads, axis=0)
        cosine, sine = rotary_tables(0, length_all)
        grad_joint = jnp.concatenate(
            [
                rotate_back(grad_query, cosine, sine),
                rotate_back(grad_keys, cosine, sine),
                grad_values,
            ],
            axis=-1,
        ).astype(jnp.bfloat16)
        inner = (grad_qkv, grad_qkv_bias, gain_one, shift_one)
        outputs = []
        for index in range(blocks):
            start = index * BLOCK

            def work_norm(operand, start=start):
                grad_qkv_now, grad_bias_now, gain_now, shift_now = operand
                values32 = row_tokens[start : start + BLOCK].astype(jnp.float32)
                normed, unit, inverse = layer_norm_parts(values32, first_gain, first_shift)
                grad_rows = grad_joint[start : start + BLOCK]
                grad_qkv_now = grad_qkv_now + jnp.einsum(
                    "bhe,bd->hed",
                    grad_rows,
                    normed.astype(jnp.bfloat16),
                    preferred_element_type=jnp.float32,
                )
                grad_bias_now = grad_bias_now + jnp.sum(grad_rows.astype(jnp.float32), axis=0)
                grad_normed = jnp.einsum(
                    "bhe,hed->bd", grad_rows, qkv_back, preferred_element_type=jnp.float32
                )
                gain_now = gain_now + jnp.sum(grad_normed * unit, axis=0)
                shift_now = shift_now + jnp.sum(grad_normed, axis=0)
                return (
                    (grad_qkv_now, grad_bias_now, gain_now, shift_now),
                    norm_back(grad_normed, unit, inverse, first_gain),
                )

            inner, piece = lax.cond(
                start < length,
                work_norm,
                lambda operand: (operand, jnp.zeros((BLOCK, width), jnp.float32)),
                inner,
            )
            outputs.append(piece)
        grad_qkv, grad_qkv_bias, gain_one, shift_one = inner
        return (
            (grad_qkv, grad_qkv_bias, grad_dense, gain_one, shift_one),
            jnp.concatenate(outputs, axis=0),
        )

    attention_init = (
        jnp.zeros(qkv_back.shape, jnp.float32),
        jnp.zeros((heads_here, 3 * HEAD), jnp.float32),
        jnp.zeros((heads_here * HEAD, width), jnp.float32),
        jnp.zeros((width,), jnp.float32),
        jnp.zeros((width,), jnp.float32),
    )
    attention_totals, grad_x_one = lax.scan(
        attention_back,
        attention_init,
        (tokens, grad_out, query_all, keys_all, values_all, attended_all, logsum_all, lengths),
    )
    grad_qkv_total, grad_qkv_bias_total, grad_dense_total, gain_one, shift_one = attention_totals
    grad_dense_total = grad_dense_total.reshape(heads_here, HEAD, width)
    norms_total = jnp.stack([gain_one, shift_one, gain_two, shift_two, bias_term])
    (
        qkv_grad_out,
        qkv_bias_grad_out,
        dense_grad_out,
        up_grad_out,
        up_bias_grad_out,
        down_grad_out,
        norms_dp,
    ) = (
        lax.psum_scatter(
            grad_qkv_total.astype(jnp.bfloat16), "dp", scatter_dimension=1, tiled=True
        ).astype(jnp.float32),
        lax.psum_scatter(
            grad_qkv_bias_total.astype(jnp.bfloat16), "dp", scatter_dimension=1, tiled=True
        ).astype(jnp.float32),
        lax.psum_scatter(
            grad_dense_total.astype(jnp.bfloat16), "dp", scatter_dimension=1, tiled=True
        ).astype(jnp.float32),
        lax.psum_scatter(
            grad_up_total.astype(jnp.bfloat16), "dp", scatter_dimension=0, tiled=True
        ).astype(jnp.float32),
        lax.psum_scatter(
            grad_up_bias_total.astype(jnp.bfloat16), "dp", scatter_dimension=0, tiled=True
        ).astype(jnp.float32),
        lax.psum_scatter(
            grad_down_total.astype(jnp.bfloat16), "dp", scatter_dimension=0, tiled=True
        ).astype(jnp.float32),
        lax.psum_scatter(
            norms_total.astype(jnp.bfloat16), "dp", scatter_dimension=1, tiled=True
        ).astype(jnp.float32),
    )
    grad_x_partial = grad_x_one + grad_x_two
    grad_x_total, norms_out = (
        lax.psum_scatter(grad_x_partial, "tensor", scatter_dimension=2, tiled=True),
        lax.psum_scatter(norms_dp, "tensor", scatter_dimension=1, tiled=True),
    )
    grad_slice = lax.dynamic_slice_in_dim(grad_out, column_start, slice_width, 2).astype(
        jnp.float32
    )
    input_grad = (grad_slice + grad_x_total).astype(jnp.bfloat16)
    return (
        block_out,
        input_grad,
        qkv_grad_out,
        qkv_bias_grad_out,
        dense_grad_out,
        up_grad_out,
        up_bias_grad_out,
        down_grad_out,
        norms_out,
    )


F32 = jnp.float32
LOW = jnp.bfloat16
ROWS = 512
PARTS = 4
VMEM_LIMIT = 60 * 1024 * 1024


def dot_nt(left, right):
    return lax.dot_general(left, right, (((1,), (1,)), ((), ())), preferred_element_type=F32)


def dot_nn(left, right):
    return lax.dot_general(left, right, (((1,), (0,)), ((), ())), preferred_element_type=F32)


def dot_tn(left, right):
    return lax.dot_general(left, right, (((0,), (0,)), ((), ())), preferred_element_type=F32)


def whole(shape):
    return pl.BlockSpec(shape, lambda *_: (0,) * len(shape), pipeline_mode=pl.Buffered(1))


def params(dims=1):
    return pltpu.CompilerParams(
        dimension_semantics=("arbitrary",) * dims, vmem_limit_bytes=VMEM_LIMIT
    )


def cost(flops, nbytes, exps=0):
    return pl.CostEstimate(flops=flops, bytes_accessed=nbytes, transcendentals=exps)


def row_block(width):
    return pl.BlockSpec((ROWS, width), lambda b, *_: (b, 0))


def block_live(lens_ref, length_all):
    per_seq = length_all // ROWS
    b = pl.program_id(0)
    return (b % per_seq) * ROWS < lens_ref[b // per_seq]


def seq_block(width, length_all, seq):
    return pl.BlockSpec((ROWS, width), lambda b, *_: (b + seq * (length_all // ROWS), 0))


def unit_rows(values):
    values = values.astype(F32)
    centred = values - jnp.mean(values, axis=-1, keepdims=True)
    inverse = lax.rsqrt(jnp.mean(centred * centred, axis=-1, keepdims=True) + 1e-05)
    return centred * inverse, inverse


def norms_kernel(tokens_ref, grad_ref, valid_ref, affine_ref, *refs):
    normed_ref, mixed_ref, out_ref = refs[-3:]

    unit, _ = unit_rows(tokens_ref[...])
    normed_ref[...] = (unit * affine_ref[0:1, :] + affine_ref[1:2, :]).astype(LOW)
    mixed_ref[...] = (unit * affine_ref[2:3, :] + affine_ref[3:4, :]).astype(LOW)
    out_ref[...] = (grad_ref[...].astype(F32) * valid_ref[...]).astype(LOW)


def both_norms(tokens, cotangent, valid, affine, into, index):
    rows, width = tokens.shape
    steps = rows // 256
    out = jax.ShapeDtypeStruct((2 * rows, width), LOW)
    spec = pl.BlockSpec((256, width), lambda b: (b, 0))
    return pl.pallas_call(
        norms_kernel,
        grid=(steps,),
        in_specs=[spec, spec, pl.BlockSpec((256, 1), lambda b: (b, 0)), whole((8, width))]
        + [pl.BlockSpec(memory_space=pl.ANY)] * len(into),
        out_specs=[pl.BlockSpec((256, width), lambda b: (b + index * steps, 0))] * 3,
        out_shape=[out] * 3,
        input_output_aliases={4 + k: k for k in range(len(into))},
        compiler_params=params(),
        cost_estimate=cost(20 * rows * width, 10 * rows * width),
    )(tokens, cotangent, valid, affine, *into)


def turn_forward(values, cosine, after, before):
    part = values[:, :128]
    part = part * cosine + pltpu.roll(part, 32, 1) * after + pltpu.roll(part, 96, 1) * before
    return jnp.concatenate([part, values[:, 128:]], axis=1)


def turn_back(grad, cosine, after, before):
    part = grad[:, :128]
    part = part * cosine - pltpu.roll(part, 96, 1) * before - pltpu.roll(part, 32, 1) * after
    return jnp.concatenate([part, grad[:, 128:]], axis=1)


SLABS = ((0, (0, 1)), (1, (0, 1)), (2, (0, 1)), (3, (0,)), (3, (1,)))
SINGLE_SLABS = tuple((bits, (slab,)) for bits in range(4) for slab in range(2))


def project_kernel(chip_ref, *refs):
    normed_ref, grad_ref, bias_ref, cos_ref, after_ref, before_ref = refs[:6]
    slot_refs = refs[6:11]
    query_ref, grad_attended_ref, weight_ref, dense_ref = refs[11:]
    chip = chip_ref[0]
    rows_of_head = weight_ref.shape[0] // 8
    rows_of_dense = dense_ref.shape[0] // 8

    @pl.when(pl.program_id(0) == 0)
    def _():
        for ref, (bits, slabs) in zip(slot_refs, SLABS):
            for k, slab in enumerate(slabs):
                at = jnp.bitwise_xor(chip, bits) * 2 + slab
                head_at = pl.multiple_of(at * rows_of_head, 32)
                dense_at = pl.multiple_of(at * rows_of_dense, 32)
                weight_ref[pl.ds(head_at, rows_of_head), :] = ref[k, :rows_of_head, :]
                dense_ref[pl.ds(dense_at, rows_of_dense), :] = ref[k, rows_of_head:, :]

    joint = dot_nt(normed_ref[...], weight_ref[...]) + bias_ref[0:1, :]
    tables = (cos_ref[...], after_ref[...], before_ref[...])
    query_ref[:, :HEAD] = turn_forward(joint[:, :HEAD], *tables).astype(LOW)
    query_ref[:, HEAD : 2 * HEAD] = turn_forward(joint[:, HEAD : 2 * HEAD], *tables).astype(LOW)
    query_ref[:, 2 * HEAD :] = joint[:, 2 * HEAD :].astype(LOW)
    grad_attended_ref[...] = dot_nt(grad_ref[...], dense_ref[...]).astype(LOW)


def project(chip, normed, grad_out, bias, tables, slots, length_all):
    rows, width = normed.shape
    per_seq = length_all // ROWS
    table = pl.BlockSpec((ROWS, 128), lambda b, *_: (b % per_seq, 0))
    shapes = [
        jax.ShapeDtypeStruct((rows, 3 * HEAD), LOW),
        jax.ShapeDtypeStruct((rows, HEAD), LOW),
        jax.ShapeDtypeStruct((3 * HEAD, width), LOW),
        jax.ShapeDtypeStruct((HEAD, width), LOW),
    ]
    return pl.pallas_call(
        project_kernel,
        grid_spec=pltpu.PrefetchScalarGridSpec(
            num_scalar_prefetch=1,
            grid=(rows // ROWS,),
            in_specs=[row_block(width), row_block(width), whole((8, 3 * HEAD))]
            + [table] * 3
            + [whole(slot.shape) for slot in slots],
            out_specs=[row_block(3 * HEAD), row_block(HEAD)]
            + [whole((3 * HEAD, width)), whole((HEAD, width))],
        ),
        out_shape=shapes,
        compiler_params=params(),
        cost_estimate=cost(8 * rows * width * HEAD, 4 * rows * width + 16 * HEAD * width),
        name="pr",
    )(chip, normed, grad_out, bias, *tables, *slots)


def head_grads_kernel(chip_ref, *refs):
    grad_joint_ref, attended_ref, normed_ref, grad_ref = refs[:4]
    slot_refs = refs[4:12]
    head_acc, dense_acc = refs[12:]
    chip = chip_ref[0]
    rows_of_head = head_acc.shape[0] // 8
    rows_of_dense = dense_acc.shape[0] // 8
    b = pl.program_id(0)

    @pl.when(b == 0)
    def _():
        head_acc[...] = jnp.zeros_like(head_acc)
        dense_acc[...] = jnp.zeros_like(dense_acc)

    head_acc[...] += dot_tn(grad_joint_ref[...], normed_ref[...])
    dense_acc[...] += dot_tn(attended_ref[...], grad_ref[...])

    @pl.when(b == pl.num_programs(0) - 1)
    def _():
        for ref, (bits, slabs) in zip(slot_refs, SINGLE_SLABS):
            for k, slab in enumerate(slabs):
                at = jnp.bitwise_xor(chip, bits) * 2 + slab
                head_at = pl.multiple_of(at * rows_of_head, 32)
                dense_at = pl.multiple_of(at * rows_of_dense, 32)
                ref[k, :rows_of_head, :] = head_acc[pl.ds(head_at, rows_of_head), :].astype(LOW)
                ref[k, rows_of_head:, :] = dense_acc[pl.ds(dense_at, rows_of_dense), :].astype(LOW)


def head_grads(chip, grad_joint, attended, normed, grad_out):
    rows, width = normed.shape
    slab = (1, HEAD // 2, width)
    return pl.pallas_call(
        head_grads_kernel,
        grid_spec=pltpu.PrefetchScalarGridSpec(
            num_scalar_prefetch=1,
            grid=(rows // ROWS,),
            in_specs=[row_block(3 * HEAD), row_block(HEAD), row_block(width), row_block(width)],
            out_specs=[whole(slab)] * 8,
            scratch_shapes=[pltpu.VMEM((3 * HEAD, width), F32), pltpu.VMEM((HEAD, width), F32)],
        ),
        out_shape=[jax.ShapeDtypeStruct(slab, LOW)] * 8,
        compiler_params=params(),
        cost_estimate=cost(8 * rows * width * HEAD, 4 * rows * width + 8 * HEAD * width),
        name="hg",
    )(chip, grad_joint, attended, normed, grad_out)


def attention_kernel(
    lens_ref,
    query_ref,
    grad_ref,
    cos_ref,
    after_ref,
    before_ref,
    attended_ref,
    grad_joint_ref,
    bias_ref,
    grad_key_s,
    grad_value_s,
):
    seq = pl.program_id(0)
    length = lens_ref[seq]
    length_all = query_ref.shape[0]
    tile = 256
    scale = HEAD ** (-0.5)
    grad_key_s[...] = jnp.zeros_like(grad_key_s)
    grad_value_s[...] = jnp.zeros_like(grad_value_s)

    @pl.when(seq == 0)
    def _():
        bias_ref[...] = jnp.zeros_like(bias_ref)

    for start in range(0, length_all, tile):
        rows = slice(start, start + tile)
        extent = start + tile

        @pl.when(start < length)
        def _(rows=rows, extent=extent, start=start):
            query = query_ref[rows, :HEAD]
            keys = query_ref[:extent, HEAD : 2 * HEAD]
            values = query_ref[:extent, 2 * HEAD :]
            grad = grad_ref[rows, :]
            scores = dot_nt(query, keys) * scale
            row_id = start + lax.broadcasted_iota(jnp.int32, scores.shape, 0)
            column_id = lax.broadcasted_iota(jnp.int32, scores.shape, 1)
            allowed = (column_id <= row_id) & (column_id < length)
            scores = jnp.where(allowed, scores, -1e30)
            weights = jnp.exp(scores - jnp.max(scores, axis=-1, keepdims=True))
            probs = weights / jnp.sum(weights, axis=-1, keepdims=True)
            probs_low = probs.astype(LOW)
            attended_ref[rows, :] = dot_nn(probs_low, values).astype(LOW)
            grad_probs = dot_nt(grad, values)
            delta = jnp.sum(probs * grad_probs, axis=-1, keepdims=True)
            grad_scores = (probs * (grad_probs - delta)).astype(LOW)
            tables = (cos_ref[rows, :], after_ref[rows, :], before_ref[rows, :])
            grad_query = turn_back(dot_nn(grad_scores, keys) * scale, *tables).astype(LOW)
            grad_joint_ref[rows, :HEAD] = grad_query
            grad_key_s[:extent, :] += dot_tn(grad_scores, query)
            grad_value_s[:extent, :] += dot_tn(probs_low, grad)
            bias_ref[0:1, :HEAD] += jnp.sum(grad_query.astype(F32), axis=0, keepdims=True)

        @pl.when(start >= length)
        def _(rows=rows):
            attended_ref[rows, :] = jnp.zeros((tile, HEAD), LOW)
            grad_joint_ref[rows, :HEAD] = jnp.zeros((tile, HEAD), LOW)

    for start in range(0, length_all, tile):
        rows = slice(start, start + tile)
        tables = (cos_ref[rows, :], after_ref[rows, :], before_ref[rows, :])
        grad_key = turn_back(grad_key_s[rows, :] * scale, *tables).astype(LOW)
        grad_value = grad_value_s[rows, :].astype(LOW)
        grad_joint_ref[rows, HEAD : 2 * HEAD] = grad_key
        grad_joint_ref[rows, 2 * HEAD :] = grad_value
        bias_ref[0:1, HEAD : 2 * HEAD] += jnp.sum(grad_key.astype(F32), axis=0, keepdims=True)
        bias_ref[0:1, 2 * HEAD :] += jnp.sum(grad_value.astype(F32), axis=0, keepdims=True)


def attention_both(lens, joint, grad_attended, tables, length_all):
    rows = joint.shape[0]
    seqs = rows // length_all

    def per_seq(width):
        return pl.BlockSpec((length_all, width), lambda s, *_: (s, 0))

    return pl.pallas_call(
        attention_kernel,
        grid_spec=pltpu.PrefetchScalarGridSpec(
            num_scalar_prefetch=1,
            grid=(seqs,),
            in_specs=[per_seq(3 * HEAD), per_seq(HEAD)] + [whole((length_all, 128))] * 3,
            out_specs=[per_seq(HEAD), per_seq(3 * HEAD), whole((8, 3 * HEAD))],
            scratch_shapes=[pltpu.VMEM((length_all, HEAD), F32)] * 2,
        ),
        out_shape=[
            jax.ShapeDtypeStruct((rows, HEAD), LOW),
            jax.ShapeDtypeStruct((rows, 3 * HEAD), LOW),
            jax.ShapeDtypeStruct((8, 3 * HEAD), F32),
        ],
        compiler_params=params(),
        cost_estimate=cost(12 * rows * length_all * HEAD, 14 * rows * HEAD, rows * length_all),
        name="attention_both",
    )(lens, joint, grad_attended, *tables)


def feed_kernel(length_all, pieces, lens_ref, *refs):
    mixed_ref, grad_ref, bias_ref = refs[:3]
    piece_refs = refs[3 : 3 + pieces]
    active_ref, grad_hidden_ref, bias_grad_ref = refs[3 + pieces : 6 + pieces]
    out_refs = refs[6 + pieces : 6 + 2 * pieces]
    up_s, down_s, up_acc, down_acc = refs[6 + 2 * pieces :]
    b = pl.program_id(0)

    @pl.when(b == 0)
    def _():
        at = 0
        for ref in piece_refs:
            for half in range(ref.shape[0]):
                up_s[at : at + 128, :] = ref[half, 0]
                down_s[at : at + 128, :] = ref[half, 1]
                at += 128
        up_acc[...] = jnp.zeros_like(up_acc)
        down_acc[...] = jnp.zeros_like(down_acc)
        bias_grad_ref[...] = jnp.zeros_like(bias_grad_ref)

    live = block_live(lens_ref, length_all)

    @pl.when(live)
    def _():
        mixed = mixed_ref[...]
        grad = grad_ref[...]
        hidden = dot_nt(mixed, up_s[...]) + bias_ref[0:1, :]
        gate = 0.5 * (1.0 + lax.erf(hidden * (2.0**-0.5)))
        active = (hidden * gate).astype(LOW)
        slope = gate + hidden * jnp.exp(-0.5 * hidden * hidden) * 0.3989422804014327
        grad_hidden32 = dot_nt(grad, down_s[...]) * slope
        grad_hidden = grad_hidden32.astype(LOW)
        active_ref[...] = active
        grad_hidden_ref[...] = grad_hidden
        bias_grad_ref[0:1, :] += jnp.sum(grad_hidden.astype(F32), axis=0, keepdims=True)
        down_acc[...] += dot_tn(active, grad)
        up_acc[...] += dot_tn(grad_hidden, mixed)

    @pl.when(jnp.logical_not(live))
    def _():
        active_ref[...] = jnp.zeros_like(active_ref)
        grad_hidden_ref[...] = jnp.zeros_like(grad_hidden_ref)

    @pl.when(b == pl.num_programs(0) - 1)
    def _():
        at = 0
        for ref in out_refs:
            for half in range(ref.shape[0]):
                ref[half, 0] = up_acc[at : at + 128, :].astype(LOW)
                ref[half, 1] = down_acc[at : at + 128, :].astype(LOW)
                at += 128


def feed_part(lens, mixed, grad_out, bias, pieces, length_all):
    rows, width = mixed.shape
    units = sum(128 * piece.shape[0] for piece in pieces)
    out = pl.pallas_call(
        partial(feed_kernel, length_all, len(pieces)),
        grid_spec=pltpu.PrefetchScalarGridSpec(
            num_scalar_prefetch=1,
            grid=(rows // ROWS,),
            in_specs=[row_block(width), row_block(width), whole((8, units))]
            + [whole(piece.shape) for piece in pieces],
            out_specs=[row_block(units), row_block(units), whole((8, units))]
            + [whole(piece.shape) for piece in pieces],
            scratch_shapes=[pltpu.VMEM((units, width), LOW)] * 2
            + [pltpu.VMEM((units, width), F32)] * 2,
        ),
        out_shape=[
            jax.ShapeDtypeStruct((rows, units), LOW),
            jax.ShapeDtypeStruct((rows, units), LOW),
            jax.ShapeDtypeStruct((8, units), F32),
        ]
        + [jax.ShapeDtypeStruct(piece.shape, LOW) for piece in pieces],
        compiler_params=params(),
        cost_estimate=cost(
            8 * rows * width * units, 4 * rows * width + 8 * units * width, 2 * rows * units
        ),
    )(lens, mixed, grad_out, jnp.broadcast_to(bias.astype(F32)[None, :], (8, units)), *pieces)
    return out[0], out[1], out[2][0], out[3:]


def output_kernel(seq, parts, pieces, lens_ref, *refs):
    active_refs = refs[: parts + 1]
    dense_ref = refs[parts + 1]
    piece_refs = refs[parts + 2 : parts + 2 + pieces]
    out_ref, down_s = refs[parts + 2 + pieces :]

    @pl.when(pl.program_id(0) == 0)
    def _():
        at = 0
        for ref in piece_refs:
            for half in range(ref.shape[0]):
                down_s[at : at + 128, :] = ref[half, 1]
                at += 128
        down_s[at : at + HEAD, :] = dense_ref[...]

    live = pl.program_id(0) * ROWS < lens_ref[seq]

    @pl.when(live)
    def _():
        left = jnp.concatenate([ref[...] for ref in active_refs], axis=1)
        out_ref[...] = dot_nn(left, down_s[...]).astype(LOW)

    @pl.when(jnp.logical_not(live))
    def _():
        out_ref[...] = jnp.zeros_like(out_ref)


def branch_output(lens, actives, attended, dense, pieces, length_all, seq):
    rows, width = length_all, dense.shape[1]
    units = sum(active.shape[1] for active in actives)
    return pl.pallas_call(
        partial(output_kernel, seq, len(actives), len(pieces)),
        grid_spec=pltpu.PrefetchScalarGridSpec(
            num_scalar_prefetch=1,
            grid=(rows // ROWS,),
            in_specs=[seq_block(active.shape[1], length_all, seq) for active in actives]
            + [seq_block(HEAD, length_all, seq), whole(dense.shape)]
            + [whole(piece.shape) for piece in pieces],
            out_specs=row_block(width),
            scratch_shapes=[pltpu.VMEM((units + HEAD, width), LOW)],
        ),
        out_shape=jax.ShapeDtypeStruct((rows, width), LOW),
        compiler_params=params(),
        cost_estimate=cost(
            2 * rows * width * (units + HEAD), 2 * rows * (width + units) + 4 * units * width
        ),
    )(lens, *actives, attended, dense, *pieces)


def swap(value, bit):
    size = lax.axis_size("dp")
    return lax.ppermute(value, "dp", [(k, k ^ bit) for k in range(size)])


def add_low(*terms):
    total = terms[0].astype(F32)
    for term in terms[1:]:
        total = total + term.astype(F32)
    return total


def chain_steps(parts, one_ref, two_ref, out_ref, sent_s, got_s, send_sems, recv_sems):
    size = lax.axis_size("tensor")
    here = lax.axis_index("tensor")
    rows, width = out_ref.shape[0] // parts, out_ref.shape[1]
    total = (size - 1) * parts
    below, above = here > 0, here < size - 1
    up, down = lax.min(here + 1, size - 1), lax.max(here - 1, 0)
    mesh_id = pl.DeviceIdType.MESH

    def copy(way, item):
        return pltpu.make_async_remote_copy(
            src_ref=sent_s.at[way, item],
            dst_ref=got_s.at[way, item],
            send_sem=send_sems.at[way, item],
            recv_sem=recv_sems.at[way, item],
            device_id={"tensor": down if way else up},
            device_id_type=mesh_id,
        )

    def own(shard, part):
        at = (
            pl.ds(pl.multiple_of(part * rows, rows), rows),
            pl.ds(pl.multiple_of(shard * width, width), width),
        )
        return one_ref[at].astype(F32) + two_ref[at].astype(F32)

    def shard_of(way, item):
        turn = item // parts
        return turn if way else size - 1 - turn

    def sends(way, item):
        shard = shard_of(way, item)
        return (item >= 0) & (item < total) & ((shard < here) if way else (shard > here))

    def greet():
        barrier = pltpu.get_barrier_semaphore()

        @pl.when(below)
        def _():
            pl.semaphore_signal(barrier, inc=1, device_id={"tensor": down}, device_id_type=mesh_id)

        @pl.when(above)
        def _():
            pl.semaphore_signal(barrier, inc=1, device_id={"tensor": up}, device_id_type=mesh_id)

        pl.semaphore_wait(barrier, lax.select(below & above, jnp.int32(2), jnp.int32(1)))

    def step(time, unused):
        for way in range(2):
            first = above if way else below
            item = time - (size - 1 - here if way else here)

            @pl.when(sends(way, item))
            def _(way=way, item=item, first=first):
                part = item % parts
                value = own(shard_of(way, item), part)

                @pl.when(first)
                def _():
                    copy(way, item).wait_recv()
                    sent_s[way, item] = (value + got_s[way, item].astype(F32)).astype(LOW)

                @pl.when(jnp.logical_not(first))
                def _():
                    sent_s[way, item] = value.astype(LOW)

                copy(way, item).start()

        return unused

    def finish(part, unused):
        at = pl.ds(pl.multiple_of(part * rows, rows), rows)
        out_ref[at, :] = own(here, part)
        for way in range(2):
            turn = here if way else size - 1 - here

            @pl.when(above if way else below)
            def _(way=way, turn=turn):
                item = turn * parts + part
                copy(way, item).wait_recv()
                out_ref[at, :] += got_s[way, item].astype(F32)

        return unused

    def drain(item, unused):
        for way in range(2):

            @pl.when(sends(way, item))
            def _(way=way):
                copy(way, item).wait_send()

        return unused

    def close(start):
        lax.fori_loop(start, total + size - 1, step, 0)
        lax.fori_loop(0, parts, finish, 0)
        lax.fori_loop(0, total, drain, 0)

    return greet, step, close


def chain_kernel(parts, one_ref, two_ref, *refs):
    sum_refs, (out_ref, up_ref, down_ref) = refs[:6], refs[6:9]
    greet, step, close = chain_steps(parts, one_ref, two_ref, out_ref, *refs[9:])
    greet()
    step(0, 0)
    for half in range(2):
        own, over_x, over_y = sum_refs[3 * half : 3 * half + 3]
        for kind, ref in enumerate((up_ref, down_ref)):
            at = slice(half * 128, half * 128 + 128)
            ref[at, :] = own[0, kind].astype(F32) + over_x[0, kind].astype(F32)
            ref[at, :] += over_y[0, kind].astype(F32)
    close(1)


def chain_scratch(rows, width):
    size = lax.axis_size("tensor")
    slots = (2, (size - 1) * PARTS, rows // PARTS, width // size)
    return [
        pltpu.VMEM(slots, LOW),
        pltpu.VMEM(slots, LOW),
        pltpu.SemaphoreType.DMA(slots[:2]),
        pltpu.SemaphoreType.DMA(slots[:2]),
    ]


def input_grads_kernel(parts, pieces, *refs):
    grad_refs = refs[:parts]
    grad_joint_ref, own_ref, other_ref, affine_ref, qkv_ref = refs[parts : parts + 5]
    piece_refs = refs[parts + 5 : parts + 5 + pieces]
    rest = refs[parts + 5 + pieces :]
    branch_refs, (out_own_ref, out_other_ref, norm_ref, total_ref) = rest[:2], rest[2:6]
    up_s, one_s, two_s = rest[6:9]
    greet, step, close = chain_steps(PARTS, *branch_refs, total_ref, *rest[9:])
    b = pl.program_id(0)
    steps = pl.num_programs(0)

    @pl.when(b == 0)
    def _():
        greet()

    step(b, 0)

    @pl.when(b == 0)
    def _():
        for k, ref in enumerate(piece_refs):
            up_s[128 * k : 128 * k + 128, :] = ref[0, 0]
        norm_ref[...] = jnp.zeros_like(norm_ref)

    one_s[...] = dot_nn(grad_joint_ref[...], qkv_ref[...])
    left = jnp.concatenate([ref[...] for ref in grad_refs], axis=1)
    two_s[...] = dot_nn(left, up_s[...])
    is_other = b < steps // 2
    unit, inverse = unit_rows(jnp.where(is_other, other_ref[...], own_ref[...]))
    grad_one, grad_two = one_s[...], two_s[...]
    first, second = grad_one * unit, grad_two * unit
    norm_ref[0:1, :] += jnp.sum(first, axis=0, keepdims=True)
    norm_ref[1:2, :] += jnp.sum(grad_one, axis=0, keepdims=True)
    norm_ref[2:3, :] += jnp.sum(second, axis=0, keepdims=True)
    norm_ref[3:4, :] += jnp.sum(grad_two, axis=0, keepdims=True)
    gain_one, gain_two = affine_ref[0:1, :], affine_ref[2:3, :]
    scaled = grad_one * gain_one + grad_two * gain_two
    along = jnp.mean(first * gain_one + second * gain_two, axis=-1, keepdims=True)
    scaled_mean = jnp.mean(scaled, axis=-1, keepdims=True)
    result = (inverse * (scaled - scaled_mean - unit * along)).astype(LOW)

    @pl.when(is_other)
    def _():
        out_other_ref[...] = result

    @pl.when(jnp.logical_not(is_other))
    def _():
        out_own_ref[...] = result

    @pl.when(b == steps - 1)
    def _():
        close(steps)


def input_grads_and_chain(grads, grad_joint, own, other, affine, qkv, pieces, branches):
    rows, width = own.shape
    size = lax.axis_size("tensor")
    block = 256
    half = rows // block
    units = sum(grad.shape[1] for grad in grads)

    def turned(columns):
        return pl.BlockSpec((block, columns), lambda b: ((b + half) % (2 * half), 0))

    def own_block():
        return pl.BlockSpec((block, width), lambda b: (jnp.maximum(b - half, 0), 0))

    def other_block():
        return pl.BlockSpec((block, width), lambda b: (jnp.minimum(b, half - 1), 0))

    piece_spec = pl.BlockSpec(
        (1, 1, 128, width), lambda b: (0, 0, 0, 0), pipeline_mode=pl.Buffered(1)
    )
    return pl.pallas_call(
        partial(input_grads_kernel, len(grads), len(pieces)),
        grid=(2 * half,),
        in_specs=[turned(grad.shape[1]) for grad in grads]
        + [turned(3 * HEAD), own_block(), other_block(), whole((8, width)), whole(qkv.shape)]
        + [piece_spec] * len(pieces)
        + [whole((rows, width))] * 2,
        out_specs=[own_block(), other_block(), whole((8, width)), whole((rows, width // size))],
        out_shape=[
            jax.ShapeDtypeStruct((rows, width), LOW),
            jax.ShapeDtypeStruct((rows, width), LOW),
            jax.ShapeDtypeStruct((8, width), F32),
            jax.ShapeDtypeStruct((rows, width // size), F32),
        ],
        scratch_shapes=[pltpu.VMEM((units, width), LOW)]
        + [pltpu.VMEM((block, width), F32)] * 2
        + chain_scratch(rows, width),
        compiler_params=pltpu.CompilerParams(
            dimension_semantics=("arbitrary",),
            collective_id=1,
            has_side_effects=True,
            vmem_limit_bytes=64 * 1024 * 1024 - 65536,
        ),
        cost_estimate=cost(4 * rows * width * (units + 3 * HEAD), 16 * rows * width),
    )(*grads, grad_joint, own, other, affine, qkv, *pieces, *branches)


def chain_in_kernel(one, two, sums):
    size = lax.axis_size("tensor")
    rows, width = one.shape
    return pl.pallas_call(
        partial(chain_kernel, PARTS),
        in_specs=[pl.BlockSpec(memory_space=pltpu.VMEM)] * (2 + len(sums)),
        out_specs=[pl.BlockSpec(memory_space=pltpu.VMEM)] * 3,
        out_shape=[jax.ShapeDtypeStruct((rows, width // size), F32)]
        + [jax.ShapeDtypeStruct((2 * sums[0].shape[2], width), F32)] * 2,
        scratch_shapes=chain_scratch(rows, width),
        compiler_params=pltpu.CompilerParams(
            collective_id=0, has_side_effects=True, vmem_limit_bytes=VMEM_LIMIT
        ),
        cost_estimate=cost(2 * rows * width, 8 * rows * width),
    )(one, two, *sums)


def small_scatter(value, axis, bits):
    place = lax.axis_index(axis)
    size = lax.axis_size(axis)
    for bit in bits:
        half = value.shape[0] // 2
        upper = (place // bit) % 2
        mine = lax.dynamic_slice_in_dim(value, upper * half, half, 0)
        theirs = lax.dynamic_slice_in_dim(value, (1 - upper) * half, half, 0)
        value = mine + lax.ppermute(theirs, axis, [(k, k ^ bit) for k in range(size)])
    return value[0]


def local_fast(
    tokens,
    cotangent,
    lengths,
    keep,
    first_gain,
    first_shift,
    second_gain,
    second_shift,
    qkv_weight,
    qkv_bias,
    dense_weight,
    up_weight,
    up_bias,
    down_weight,
    branch_bias,
):
    tokens, cotangent, keep = tokens[0], cotangent[0], keep[0]
    length_all, width = tokens.shape
    place = lax.axis_index("dp")
    core, chip = place % 2, place // 2
    dp_size, tensor_size = lax.axis_size("dp"), lax.axis_size("tensor")
    qkv_rows, units = qkv_weight.shape[1], up_weight.shape[0]
    positions = jnp.arange(length_all)
    live = positions < lengths[0]
    valid = (live & (keep == 1)).astype(F32)
    chips = chip.astype(jnp.int32)[None]

    def head_rows(head):
        return jnp.concatenate(
            [
                lax.dynamic_index_in_dim(qkv_weight, head, 0, False),
                lax.dynamic_index_in_dim(dense_weight, head, 0, False),
            ],
            axis=0,
        )

    def by_core(mine, other):
        pair = jnp.zeros((2,) + mine.shape, mine.dtype)
        pair = lax.dynamic_update_index_in_dim(pair, mine, core, 0)
        return lax.dynamic_update_index_in_dim(pair, other, 1 - core, 0)

    head_own = by_core(head_rows(core), swap(head_rows(1 - core), 1))
    head_x, head_y = swap(head_own, 2), swap(head_own, 4)
    head_d0, head_d1 = swap(head_y[:1], 2), swap(head_x[1:], 4)
    slots = (head_own, head_x, head_y, head_d0, head_d1)

    other_tokens = swap(tokens, 1)
    other_cotangent = swap(cotangent, 1)
    facts = jnp.concatenate([valid, jnp.full((128,), 1.0, F32) * lengths[0].astype(F32)])[None]
    other_facts = swap(facts, 1)
    lens = jnp.stack([lengths[0], other_facts[0, length_all].astype(jnp.int32)])
    affine = jnp.stack([first_gain, first_shift, second_gain, second_shift] * 2)
    firsts = both_norms(tokens, cotangent, valid[:, None], affine, (), 0)
    positions, _ = lax.optimization_barrier((positions, firsts[0]))
    biases = jnp.concatenate([up_bias, qkv_bias.reshape(-1)])
    biases = jnp.pad(biases, (0, -biases.shape[0] % 128))[None]
    for bit in (1, 2, 4):
        biases = jnp.concatenate([biases, swap(biases, bit)], axis=0)
    up_biases = biases[:, :units]
    qkv_biases = biases[:, units : units + 2 * qkv_rows].reshape(dp_size, 2, qkv_rows)
    qkv_biases = lax.dynamic_index_in_dim(qkv_biases, core, 1, False)
    qkv_bias_head = qkv_biases[place ^ jnp.arange(dp_size)].reshape(-1).astype(F32)
    qkv_bias_head = jnp.broadcast_to(qkv_bias_head[None], (8, 3 * HEAD))

    normed, mixed, grad_out = both_norms(
        other_tokens, other_cotangent, other_facts[0, :length_all][:, None], affine, firsts, 1
    )

    up_halves = up_weight.reshape(2, 1, units // 2, width)
    down_halves = down_weight.reshape(2, 1, units // 2, width)
    feed_0 = jnp.stack([up_halves[0], down_halves[0]], axis=1)
    feed_1 = jnp.stack([up_halves[1], down_halves[1]], axis=1)
    feed_x0, feed_y0 = swap(feed_0, 2), swap(feed_0, 4)
    feed_x1, feed_y1 = swap(feed_1, 2), swap(feed_1, 4)
    feed_d0, feed_d1 = swap(feed_y0, 2), swap(feed_x1, 4)

    def feed(pieces, bias):
        bias = jnp.concatenate(bias)
        return feed_part(lens, mixed, grad_out, bias, pieces, length_all)

    low_units, high_units = slice(0, units // 2), slice(units // 2, units)
    feed_a = feed([feed_0, feed_1], [up_bias])

    cosine, sine = rotary_tables(positions[0].astype(F32), length_all)
    cosine, sine = cosine[:, 0], sine[:, 0]
    half = ROT // 2
    zeros = jnp.zeros((length_all, 128 - ROT), F32)
    blank = jnp.zeros((length_all, half), F32)
    tables = (
        jnp.concatenate([cosine, zeros + 1.0], axis=1),
        jnp.concatenate([blank, sine[:, half:], zeros], axis=1),
        jnp.concatenate([-sine[:, :half], blank, zeros], axis=1),
    )
    query_key_value, grad_attended, qkv_full, dense_full = project(
        chips, normed, grad_out, qkv_bias_head, tables, slots, length_all
    )
    attended, grad_joint, bias_joint = attention_both(
        lens, query_key_value, grad_attended, tables, length_all
    )
    slot_grads = head_grads(chips, grad_joint, attended, normed, grad_out)

    feed_b = feed(
        [feed_x0, feed_y0, feed_x1, feed_y1, feed_d0, feed_d1],
        [up_biases[2, low_units], up_biases[4, low_units]]
        + [up_biases[2, high_units], up_biases[4, high_units], up_biases[6]],
    )
    feeds = (feed_a, feed_b)
    pieces = [feed_0, feed_1, feed_x0, feed_y0, feed_x1, feed_y1, feed_d0, feed_d1]

    def branch_of(seq):
        actives = [item[0] for item in feeds]
        return branch_output(lens, actives, attended, dense_full, pieces, length_all, seq)

    branch_other = swap(branch_of(1), 1)
    branch_own = branch_of(0)

    grad_x_own, grad_x_other, norm_sums, branch_total = input_grads_and_chain(
        [item[1] for item in feeds],
        grad_joint,
        tokens,
        other_tokens,
        affine,
        qkv_full,
        pieces,
        (branch_own, branch_other),
    )
    grad_x_other = swap(grad_x_other, 1)
    slice_width = width // tensor_size
    column_start = lax.axis_index("tensor") * slice_width
    token_slice = lax.dynamic_slice_in_dim(tokens, column_start, slice_width, 1).astype(F32)
    bias_slice = lax.dynamic_slice_in_dim(branch_bias, column_start, slice_width, 0)
    block_out = (token_slice + jnp.where(live[:, None], branch_total + bias_slice, 0.0)).astype(LOW)

    def scatter(own, over_x, over_y, far):
        through_x = swap(far[0], 2)
        through_y = swap(far[1], 4)
        over_y = (add_low(over_y[0], through_x).astype(LOW), over_y[1])
        over_x = (over_x[0], add_low(over_x[1], through_y).astype(LOW))
        from_x = [swap(item, 2) for item in over_x]
        from_y = [swap(item, 4) for item in over_y]
        return [(own[k], from_x[k], from_y[k]) for k in range(2)]

    grad_a, (over_x0, over_y0, over_x1, over_y1, *far) = feed_a[3], feed_b[3]
    feed_sums = scatter(grad_a, (over_x0, over_x1), (over_y0, over_y1), far)
    grad_x_total, up_grad_out, down_grad_out = chain_in_kernel(
        grad_x_own, grad_x_other, [*feed_sums[0], *feed_sums[1]]
    )
    grad_slice = lax.dynamic_slice_in_dim(cotangent, column_start, slice_width, 1).astype(F32)
    input_grad = (grad_slice * valid[:, None] + grad_x_total).astype(LOW)

    head_sums = scatter(*[slot_grads[2 * k : 2 * k + 2] for k in range(4)])
    head_grad = jnp.concatenate([add_low(*item) for item in head_sums], axis=0)
    head_mine = lax.dynamic_index_in_dim(head_grad, core, 0, False)
    head_other = lax.dynamic_index_in_dim(head_grad, 1 - core, 0, False)
    head_other = swap(head_other.astype(LOW), 1).astype(F32)
    head_out = by_core(head_mine, head_other)
    qkv_grad_out, dense_grad_out = head_out[:, :qkv_rows], head_out[:, qkv_rows:]

    (bias_own, bias_rest, bias_joint, grad_rows), norm_sums = lax.optimization_barrier(
        ((feed_a[2], feed_b[2], bias_joint, grad_out), norm_sums)
    )
    rest = bias_rest.reshape(6, units // 2)
    column_bias = jnp.stack(
        [
            bias_own,
            jnp.concatenate([rest[0], rest[2]]),
            jnp.concatenate([rest[1], rest[3]]),
            jnp.concatenate([rest[4], rest[5]]),
        ]
    )[chip ^ jnp.arange(4)]
    column_bias = jnp.stack(
        [jnp.where(core == 0, column_bias, 0.0), jnp.where(core == 0, 0.0, column_bias)], axis=1
    ).reshape(dp_size, units)
    head_bias = bias_joint[0].reshape(dp_size, qkv_rows)
    head_bias = jnp.concatenate(
        [jnp.where(core == 0, head_bias, 0.0), jnp.where(core == 0, 0.0, head_bias)], axis=1
    )
    row_width = length_all // tensor_size
    bias_term = jnp.sum(
        lax.dynamic_slice_in_dim(
            grad_rows, lax.axis_index("tensor") * row_width, row_width, 0
        ).astype(F32),
        axis=0,
    )
    norm_rows = jnp.concatenate([norm_sums[:4], bias_term[None]], axis=0)
    norm_rows = norm_rows.reshape(5, dp_size, -1).transpose(1, 0, 2).reshape(dp_size, -1)
    small = jnp.concatenate([column_bias, head_bias, norm_rows], axis=1)
    small = jnp.pad(small, ((0, 0), (0, -small.shape[1] % 128)))
    small = small_scatter(small, "dp", (4, 2, 1))
    up_bias_grad_out = small[:units]
    qkv_bias_grad_out = small[units : units + 2 * qkv_rows].reshape(2, qkv_rows)
    at = units + 2 * qkv_rows
    norms = small[at : at + 5 * width // dp_size].reshape(5, tensor_size, -1).transpose(1, 0, 2)
    bits = [1 << k for k in reversed(range(tensor_size.bit_length() - 1))]
    norms_out = small_scatter(norms.reshape(tensor_size, -1), "tensor", bits).reshape(5, -1)
    return (
        block_out[None],
        input_grad[None],
        qkv_grad_out,
        qkv_bias_grad_out,
        dense_grad_out,
        up_grad_out,
        up_bias_grad_out,
        down_grad_out,
        norms_out,
    )


def solution(mesh):
    in_specs = (
        P("dp", None, None),
        P("dp", None, None),
        P("dp"),
        P("dp", None),
        P(),
        P(),
        P(),
        P(),
        P("tensor", "dp", None),
        P("tensor", "dp"),
        P("tensor", "dp", None),
        P(("dp", "tensor"), None),
        P(("dp", "tensor")),
        P(("dp", "tensor"), None),
        P(),
    )
    out_specs = (
        P("dp", None, "tensor"),
        P("dp", None, "tensor"),
        P("tensor", "dp", None),
        P("tensor", "dp"),
        P("tensor", "dp", None),
        P(("dp", "tensor"), None),
        P(("dp", "tensor")),
        P(("dp", "tensor"), None),
        P(None, ("dp", "tensor")),
    )

    fits = mesh.shape["dp"] == 8 and mesh.shape["tensor"] * 2 == HEADS

    def local(*items):
        return (local_fast if fits else local_general)(*items)

    return jax.shard_map(local, mesh=mesh, in_specs=in_specs, out_specs=out_specs, check_vma=False)
```
